16 devices in a mesh: dp: 2 (over z), sp: 8 (over y, x, core).
Axes of the slice: x: 2, y: 2, z: 2, core: 2. Of those that a mesh axis runs over, the one named last changes fastest.
Arguments:
- feat_p3: bfloat16 [32, 256, 80, 256], P('dp', 'sp'), parts along dimension 0
- feat_p4: bfloat16 [32, 128, 40, 256], P('dp', 'sp'), parts along dimension 0
- feat_p5: bfloat16 [32, 64, 20, 256], P('dp', 'sp'), parts along dimension 0
- feat_p6: bfloat16 [32, 32, 10, 256], P('dp', 'sp'), parts along dimension 0
- feat_p7: bfloat16 [32, 16, 5, 256], P('dp', 'sp'), parts along dimension 0
- fuse_two: float32 [5, 2], replicated
- fuse_three: float32 [3, 3], replicated
- dw_filter: bfloat16 [8, 3, 3, 256], replicated
- pw_weight: bfloat16 [8, 256, 256], replicated
- bn_scale: float32 [8, 256], replicated
- bn_bias: float32 [8, 256], replicated
Outputs:
- output 1: bfloat16 [32, 256, 80, 256], P('dp', 'sp'), parts along dimension 0
- output 2: bfloat16 [32, 128, 40, 256], P('dp', 'sp'), parts along dimension 0
- output 3: bfloat16 [32, 64, 20, 256], P('dp', 'sp'), parts along dimension 0
- output 4: bfloat16 [32, 32, 10, 256], P('dp', 'sp'), parts along dimension 0
- output 5: bfloat16 [32, 16, 5, 256], P('dp', 'sp'), parts along dimension 0
There are 2 independent parts. The reference program is written for one: setup_inputs(seed, part) draws one part's arguments, and reference() takes and returns one part's arrays. A program takes and returns all parts, laid end to end along the dimension named above; an argument that names none is the same for every part.
All inputs are finite; a program needn't handle non-finite values.
Results may differ from the reference program's by a relative error of at most 0.00876237.
Values are sent between devices in bfloat16 or wider.
A program may use at most 1 GiB of HBM per device.

```python
import jax
import jax.numpy as jnp
from jax import lax

BATCH_SIZE = 16
TOP_ROWS = 16
BASE_WIDTH = 80
CHANNELS = 256

LEVEL_ROWS = [TOP_ROWS * 16, TOP_ROWS * 8, TOP_ROWS * 4, TOP_ROWS * 2, TOP_ROWS]
LEVEL_COLS = [BASE_WIDTH, BASE_WIDTH // 2, BASE_WIDTH // 4, BASE_WIDTH // 8, BASE_WIDTH // 16]
FUSE_EPS = 1e-4


def setup_inputs(seed: int = 0, part: int = 0) -> dict:
    key = jax.random.key(seed)
    map_root, weight_root = jax.random.split(key)
    map_keys = jax.random.split(jax.random.fold_in(map_root, part), 5)
    weight_keys = jax.random.split(weight_root, 6)
    result = {}
    for level in range(5):
        shape = (BATCH_SIZE, LEVEL_ROWS[level], LEVEL_COLS[level], CHANNELS)
        result['feat_p' + str(level + 3)] = jax.random.normal(map_keys[level], shape, jnp.float32).astype(jnp.bfloat16)
    result['fuse_two'] = jax.random.uniform(weight_keys[0], (5, 2), jnp.float32, 0.5, 1.5)
    result['fuse_three'] = jax.random.uniform(weight_keys[1], (3, 3), jnp.float32, 0.5, 1.5)
    result['dw_filter'] = (jax.random.normal(weight_keys[2], (8, 3, 3, CHANNELS), jnp.float32) / 3.0).astype(jnp.bfloat16)
    result['pw_weight'] = (jax.random.normal(weight_keys[3], (8, CHANNELS, CHANNELS), jnp.float32) * CHANNELS ** -0.5).astype(jnp.bfloat16)
    result['bn_scale'] = jax.random.uniform(weight_keys[4], (8, CHANNELS), jnp.float32, 0.75, 1.75)
    result['bn_bias'] = 0.5 * jax.random.normal(weight_keys[5], (8, CHANNELS), jnp.float32)
    return result


def fast_fuse(weights, maps):
    pos_weights = jnp.maximum(weights, 0.0)
    total = sum(pos_weights[index] * maps[index].astype(jnp.float32) for index in range(len(maps)))
    return total / (jnp.sum(pos_weights) + FUSE_EPS)


def upsample(image):
    return jnp.repeat(jnp.repeat(image, 2, axis=1), 2, axis=2)


def max_down(image):
    padded = jnp.pad(image, ((0, 0), (0, 1), (0, 1), (0, 0)), constant_values=-jnp.inf)
    row_count = image.shape[1]
    col_count = image.shape[2]
    vertical = jnp.maximum(jnp.maximum(padded[:, 0:row_count:2], padded[:, 1:row_count:2]), padded[:, 2:row_count + 1:2])
    return jnp.maximum(jnp.maximum(vertical[:, :, 0:col_count:2], vertical[:, :, 1:col_count:2]), vertical[:, :, 2:col_count + 1:2])


def conv_block(fused, dw_w, pw_w, scale, bias):
    activated = jax.nn.silu(fused).astype(jnp.bfloat16)
    depth = lax.conv_general_dilated(activated.astype(jnp.float32), dw_w.astype(jnp.float32)[:, :, None, :], (1, 1), ((1, 1), (1, 1)), dimension_numbers=('NHWC', 'HWIO', 'NHWC'), feature_group_count=activated.shape[3])
    point = jnp.einsum('bhwc,cd->bhwd', depth.astype(jnp.bfloat16).astype(jnp.float32), pw_w.astype(jnp.float32))
    return (point * scale + bias).astype(jnp.bfloat16)


def reference(feat_p3, feat_p4, feat_p5, feat_p6, feat_p7, fuse_two, fuse_three, dw_filter, pw_weight, bn_scale, bn_bias):
    def run_node(index, weights, maps):
        return conv_block(fast_fuse(weights, maps), dw_filter[index], pw_weight[index], bn_scale[index], bn_bias[index])

    def one_image(maps):
        input_p3, input_p4, input_p5, input_p6, input_p7 = [image[None] for image in maps]
        inner_p6 = run_node(0, fuse_two[0], [input_p6, upsample(input_p7)])
        inner_p5 = run_node(1, fuse_two[1], [input_p5, upsample(inner_p6)])
        inner_p4 = run_node(2, fuse_two[2], [input_p4, upsample(inner_p5)])
        out_p3 = run_node(3, fuse_two[3], [input_p3, upsample(inner_p4)])
        out_p4 = run_node(4, fuse_three[0], [input_p4, inner_p4, max_down(out_p3)])
        out_p5 = run_node(5, fuse_three[1], [input_p5, inner_p5, max_down(out_p4)])
        out_p6 = run_node(6, fuse_three[2], [input_p6, inner_p6, max_down(out_p5)])
        out_p7 = run_node(7, fuse_two[4], [input_p7, max_down(out_p6)])
        return (out_p3[0], out_p4[0], out_p5[0], out_p6[0], out_p7[0])

    results = lax.map(one_image, (feat_p3, feat_p4, feat_p5, feat_p6, feat_p7))
    return (results[0], results[1], results[2], results[3], results[4])
```

```python
import functools

import jax
import jax.numpy as jnp
from jax import lax
from jax.experimental import pallas as pl
from jax.experimental.pallas import tpu as pltpu
from jax.sharding import PartitionSpec as P

f32, bf16 = jnp.float32, jnp.bfloat16
FUSE_EPS = 1e-4
B, C, H = 16, 256, 128
G = N = 4
LV = (4, 5, 6, 7)
LOW = LV[1:]
TOP, END = 4, 7
TWO, THREE = range(2), range(3)
ROWS = {3: 32, 4: 16, 5: 8, 6: 4, 7: 2}
COLS = {3: 80, 4: 40, 5: 20, 6: 10, 7: 5}
PADC = {3: 80, 4: 40, 5: 24, 6: 16, 7: 8}
TILE = 8
MESH = pl.DeviceIdType.MESH
NEG = -jnp.inf
MIB = 2 ** 20


def groups(fn):
    def body(g, _):
        fn(g)
        return g
    lax.fori_loop(0, G, body, G)


def loop(n, unroll=1):
    def run(fn):
        def body(i, _):
            fn(i)
            return i
        lax.fori_loop(0, n, body, n, unroll=unroll)
    return run


def swish(h):
    return h + h * jnp.tanh(h)


def halves(v):
    return v[:, :H], v[:, H:]


def join(v):
    return jnp.concatenate(v, axis=1)


def half(c):
    return slice(c * H, c * H + H)


def cols(W, d=0):
    return slice(TILE + d, TILE + d + W)


def coefs(two, three, k):
    w = [two[i, min(k, 4)] for i in TWO] if k < 4 or k == 7 else [three[k - 4, i] for i in THREE]
    w = [jnp.maximum(x, 0.0) for x in w]
    total = jnp.full((1, C), sum(w[1:], w[0]) + FUSE_EPS, f32)
    return [jnp.full((1, C), 0.5 * x, f32) / total for x in w]


def widen(dw_ref, DW):
    for ky in THREE:
        for kx in THREE:
            DW[3 * ky + kx] = dw_ref[ky, kx].astype(f32)


def tap(DW, k, ky, kx, c):
    return DW[3 * ky + kx, k:k + 1, half(c)]


def zero_edges(S, W):
    S[..., :TILE, :] = jnp.zeros(S.shape[:-2] + (TILE, H), f32)
    S[..., TILE + W:, :] = jnp.zeros(S.shape[:-2] + (S.shape[-2] - TILE - W, H), f32)


def expand(U, v, wc):
    for c, h in enumerate(halves(v)):
        for d in TWO:
            U[c, pl.ds(d, wc, stride=2), :] = h
    return join([U[0], U[1]])


def put_s(S, ib, s, W, h):
    v = swish(h).astype(bf16).astype(f32)
    for c, x in enumerate(halves(v)):
        S[ib, c, s, cols(W), :] = x


def conv_row(S, ib, o, W, DW, k):
    out = []
    for c in TWO:
        acc = None
        for ky in THREE:
            for kx in THREE:
                t = S[ib, c, o + ky, cols(W, kx - 1), :] * tap(DW, k, ky, kx, c)
                acc = t if acc is None else acc + t
        out.append(acc)
    return join(out).astype(bf16)


def conv_rows(S, D, rows, level, k, wts, put):
    DW, pw_ref, sc_ref, bi_ref = wts
    W, wp = COLS[level], PADC[level]
    for i, (ib, o) in enumerate(rows):
        D[i * wp:i * wp + W, :] = conv_row(S, ib, o, W, DW, k)
    m = len(rows) * wp
    r = jnp.dot(D[:m], pw_ref[k], preferred_element_type=f32)
    r = (r * sc_ref[k:k + 1] + bi_ref[k:k + 1]).astype(bf16)
    for i, (ib, o) in enumerate(rows):
        put(ib, o, r[i * wp:i * wp + W])


def hmax(PV, v, W):
    out = []
    for c, x in enumerate(halves(v.astype(f32))):
        PV[c, :W, :] = x
        a, b, d = [PV[c, pl.ds(i, W // 2, stride=2), :] for i in THREE]
        out.append(jnp.maximum(jnp.maximum(a, b), d))
    return join(out).astype(bf16)


def barrier_signal(me, last):
    sem = pltpu.get_barrier_semaphore()
    for cond, d in ((me > 0, -1), (me < last, 1)):
        @pl.when(cond)
        def _(d=d):
            pl.semaphore_signal(sem, inc=1, device_id={'sp': me + d}, device_id_type=MESH)


def barrier_wait(me, last):
    sem = pltpu.get_barrier_semaphore()
    inner = (me > 0) & (me < last)

    @pl.when(inner)
    def _():
        pl.semaphore_wait(sem, 2)

    @pl.when(jnp.logical_not(inner))
    def _():
        pl.semaphore_wait(sem, 1)


def remote(src, dst, ss, rs, dev):
    return pltpu.make_async_remote_copy(src_ref=src, dst_ref=dst, send_sem=ss, recv_sem=rs, device_id={'sp': dev}, device_id_type=MESH)


def shape(l, r):
    return (B, r, COLS[l], C)


def flipped(l):
    return (B, COLS[l], ROWS[l], C)


def vm(s, t=bf16):
    return pltpu.VMEM(s, t)


DMA = pltpu.SemaphoreType.DMA
ANY = pl.BlockSpec(memory_space=pl.ANY)
VMEM = pl.BlockSpec(memory_space=pltpu.VMEM)
SMEM = pl.BlockSpec(memory_space=pltpu.SMEM)


def struct(s):
    return jax.ShapeDtypeStruct(s, bf16)


def splitter(refs):
    it = iter(refs)

    def take(n):
        return [next(it) for _ in range(n)]
    return take


EXT = {4: 2, 5: 2, 6: 2, 7: 1}
TD = (4, 5, 6)
SLOTS = {4: 1, 5: 1, 6: 4, 7: 4}


def top_down(*refs, n_dev):
    take = splitter(refs)
    two, three, p3, p4 = take(4)
    Q = dict(zip(LOW, take(3)))
    dw_ref, pw_ref, sc_ref, bi_ref = take(4)
    Th = dict(zip(TD, take(3)))
    h3, = take(1)
    X = dict(zip(LV, take(4)))
    E, T = dict(zip(LV, take(4))), dict(zip(TD, take(3)))
    S, U, F = dict(zip(TD, take(3))), dict(zip(TD, take(3))), dict(zip(LOW, take(3)))
    D, Z, DW, ls, os, xs, s_up, r_up, s_dn, r_dn, s3, r3, zs = take(13)
    me = lax.axis_index('sp')
    last = n_dev - 1
    wts = (DW, pw_ref, sc_ref, bi_ref)
    FINE_FIRST = (7, 6, 5, 4)

    def sl(g):
        return pl.ds(g * N, N)

    def load(g):
        return pltpu.make_async_copy(p4.at[sl(g)], E[4].at[sl(g), pl.ds(EXT[4], ROWS[4])], ls.at[g])

    def src(l, g, r):
        return p4.at[sl(g), pl.ds(r, EXT[l])] if l == TOP else E[l].at[sl(g), pl.ds(EXT[l] + r, EXT[l])]

    def up(l, g):
        e = EXT[l]
        return remote(src(l, g, 0), E[l].at[sl(g), pl.ds(e + ROWS[l], e)], s_up.at[l - TOP, g], r_up.at[l - TOP, g], me - 1)

    def dn(l, g):
        e = EXT[l]
        return remote(src(l, g, ROWS[l] - e), E[l].at[sl(g), pl.ds(0, e)], s_dn.at[l - TOP, g], r_dn.at[l - TOP, g], me + 1)

    up3 = remote(p3.at[:, pl.ds(0, 1)], h3.at[:, pl.ds(1, 1)], s3.at[0], r3.at[0], me - 1)
    dn3 = remote(p3.at[:, pl.ds(ROWS[3] - 1, 1)], h3.at[:, pl.ds(0, 1)], s3.at[1], r3.at[1], me + 1)

    barrier_signal(me, last)

    @groups
    def _(g):
        load(g).start()

    for l in FINE_FIRST[:-1]:
        W, R, st = COLS[l], ROWS[l], COLS[l] + 1

        @loop(B // 2)
        def _(i):
            for d in TWO:
                b = 2 * i + d
                for w in range(W):
                    for c, v in enumerate(halves(Q[l][b, w].astype(f32))):
                        F[l][d, c, pl.ds(w, R, stride=st), :] = v
                for r in range(R):
                    E[l][b, EXT[l] + r] = join([F[l][d, c, r * st:r * st + W, :] for c in TWO]).astype(bf16)
    widen(dw_ref, DW)
    for l in TD:
        zero_edges(S[l], COLS[l])
    Z[...] = jnp.zeros(Z.shape, bf16)
    edge = [pltpu.make_async_copy(Z, h3.at[:, pl.ds(i, 1)], zs) for i in TWO]

    @pl.when(me == 0)
    def _():
        edge[0].start()
        for l in LV:
            E[l][:, :EXT[l]] = jnp.zeros(shape(l, EXT[l]), bf16)

    @pl.when(me == last)
    def _():
        edge[1].start()
        for l in LV:
            E[l][:, EXT[l] + ROWS[l]:] = jnp.zeros(shape(l, EXT[l]), bf16)

    barrier_wait(me, last)
    for cond, cp, big in ((me > 0, up, up3), (me < last, dn, dn3)):
        @pl.when(cond)
        def _(cp=cp, big=big):
            @groups
            def _(g):
                for l in FINE_FIRST:
                    cp(l, g).start()
            big.start()

    def node(l, g):
        k = 6 - l
        W, wc, R = COLS[l], COLS[l + 1], ROWS[l]
        a1, a2 = coefs(two, three, k)
        coarse = E[7] if l == 6 else T[l + 1]
        nb = SLOTS[l]

        def fill(b, ib, j, u):
            x = expand(U[l].at[u], coarse[b, j].astype(f32) * a2, wc)
            for d in TWO:
                put_s(S[l], ib, 2 * j + d, W, E[l][b, 2 * j + d].astype(f32) * a1 + x)

        @loop(N // nb)
        def _(i):
            b0 = g * N + i * nb

            def put(ib, o, v):
                T[l][b0 + ib, o] = v
            if l == TOP:
                @loop((R + 4) // 4)
                def _(j):
                    for u in TWO:
                        fill(b0, 0, 2 * j + u, u)

                @loop(3)
                def _(q):
                    conv_rows(S[l], D, [(0, q * 6 + y) for y in range(6)], l, k, wts, put)
            else:
                for ib in range(nb):
                    for j in range((R + 4) // 2):
                        fill(b0 + ib, ib, j, (ib + j) % 2)
                conv_rows(S[l], D, [(ib, o) for ib in range(nb) for o in range(R + 2)], l, k, wts, put)

        for cond, o in ((me == 0, 0), (me == last, R + 1)):
            @pl.when(cond)
            def _(o=o):
                T[l][sl(g), o:o + 1] = jnp.zeros((N, 1, W, C), bf16)

    def out(l, g):
        return pltpu.make_async_copy(T[l].at[sl(g)], Th[l].at[sl(g)], os.at[l - TOP, g])

    def xout(l):
        return pltpu.make_async_copy(E[l].at[:, pl.ds(EXT[l] - 1, 1)], X[l], xs.at[l - 4])

    def arrive(l, g):
        @pl.when(me > 0)
        def _():
            dn(l, g).wait_recv()

        @pl.when(me < last)
        def _():
            up(l, g).wait_recv()

    @groups
    def _(g):
        arrive(7, g)
        for l in (6, 5, 4):
            if l == TOP:
                load(g).wait()
            arrive(l, g)
            node(l, g)
            out(l, g).start()
    for l in LV:
        xout(l).start()

    for cond, cp, sent, got in ((me > 0, up, up3, dn3), (me < last, dn, dn3, up3)):
        @pl.when(cond)
        def _(cp=cp, sent=sent, got=got):
            @groups
            def _(g):
                for l in LV:
                    cp(l, g).wait_send()
            sent.wait_send()
            got.wait_recv()

    for cond, e in ((me == 0, edge[0]), (me == last, edge[1])):
        @pl.when(cond)
        def _(e=e):
            e.wait()
    for l in LV:
        xout(l).wait()

    @groups
    def _(g):
        for l in TD:
            out(l, g).wait()


def call_top_down(n_dev, two, three, p3, p4, qs, wts):
    scratch = [vm(shape(l, ROWS[l] + 2 * EXT[l])) for l in LV] + [vm(shape(l, ROWS[l] + 2)) for l in TD]
    scratch += [vm((SLOTS[l], 2, ROWS[l] + 4, PADC[l] + 2 * TILE, H), f32) for l in TD]
    scratch += [vm((2, 2, COLS[l], H), f32) for l in TD]
    scratch += [vm((2, 2, TILE * -(-ROWS[l] * (COLS[l] + 1) // TILE), H), f32) for l in LOW]
    scratch += [vm((24 * 16 + TILE, C)), vm(shape(3, 1)), vm((9, TILE, C), f32)]
    scratch += [DMA((G,)), DMA((3, G)), DMA((4,))] + [DMA((4, G))] * 4 + [DMA((2,))] * 2 + [DMA]
    return pl.pallas_call(
        functools.partial(top_down, n_dev=n_dev),
        out_shape=[struct(shape(l, ROWS[l] + 2)) for l in TD] + [struct(shape(3, 2))] + [struct(shape(l, 1)) for l in LV],
        in_specs=[SMEM] * 2 + [ANY] * 2 + [VMEM] * 7,
        out_specs=[ANY] * 8,
        scratch_shapes=scratch,
        compiler_params=pltpu.CompilerParams(collective_id=0, has_side_effects=True, vmem_limit_bytes=60 * MIB),
    )(two, three, p3, p4, *qs, *wts)


R3, W3 = ROWS[3], COLS[3]
RC3, WC3 = ROWS[4], COLS[4]
PB = 4
NB = RC3 // PB
K3 = 3 * C


def fine(two, three, p_ref, ph_ref, t_ref, dw_ref, pw_ref, sc_ref, bi_ref, o_ref, d_ref, h_ref, S0, S1, U, X0, X1, D0, D1, PV, WD, DW):
    R, W, RC, WC = R3, W3, RC3, WC3
    Xb, Db = (X0, X1), (D0, D1)
    a1, a2 = coefs(two, three, 3)
    b = pl.program_id(0)

    @pl.when(b == 0)
    def _():
        widen(dw_ref, DW)
        zero_edges(S0, W)
        zero_edges(S1, W)
        PV[:, W:, :] = jnp.full((2, TILE, H), NEG, f32)
        eye = lax.broadcasted_iota(jnp.int32, (H, H), 0) == lax.broadcasted_iota(jnp.int32, (H, H), 1)
        for c in TWO:
            for kx in THREE:
                for pi in TWO:
                    for po in TWO:
                        v = jnp.where(eye, tap(DW, 3, 1 + pi - po, kx, c), 0.0)
                        r0 = kx * C + pi * H
                        WD[c, r0:r0 + H, half(po)] = v.astype(bf16)

    def p1(S, tj, rows, u):
        x = expand(U.at[u], t_ref[0, tj + 1].astype(f32) * a2, WC)
        for v, si in rows:
            put_s(S, 0, si, W, v.astype(f32) * a1 + x)

    def borders(S):
        p1(S, -1, [(ph_ref[0, 0], 0)], 0)
        p1(S, RC, [(ph_ref[0, 1], R + 1)], 1)

    def act(S, k):
        for t in range(PB):
            tj = k * PB + t
            p1(S, tj, [(p_ref[0, 2 * tj + d], 2 * tj + d + 1) for d in TWO], t % 2)

    def gather(S, X, k):
        for c in TWO:
            for p in range(PB):
                for kx in THREE:
                    X[c, p * W:(p + 1) * W, kx * C:kx * C + C] = join(
                        [S[0, c, 2 * (k * PB + p) + 1 + par, cols(W, kx - 1), :] for par in TWO]).astype(bf16)

    def conv(S, X, D, k):
        for c in TWO:
            r = jnp.dot(X[c, :PB * W], WD[c], preferred_element_type=f32)
            for p in range(PB):
                for par in TWO:
                    si = 2 * (k * PB + p) + 3 * par
                    q = r[p * W:(p + 1) * W, half(par)]
                    for kx in THREE:
                        q = q + S[0, c, si, cols(W, kx - 1), :] * tap(DW, 3, 2 * par, kx, c)
                    y = 2 * p + par
                    D[y * W:(y + 1) * W, half(c)] = q.astype(bf16)

    def point(D, k):
        o = jnp.dot(D[:2 * PB * W], pw_ref[3], preferred_element_type=f32)
        o = (o * sc_ref[3:4] + bi_ref[3:4]).astype(bf16)
        for y in range(2 * PB):
            o_ref[0, 2 * PB * k + y] = o[y * W:(y + 1) * W]

    def step(Sn, Sp):
        if Sn is not None:
            borders(Sn)
        gather(Sp, Xb[0], 0)

        @loop(NB // 2)
        def _(kk):
            for u in TWO:
                k = 2 * kk + u
                point(Db[1 - u], jnp.maximum(k - 1, 0))
                conv(Sp, Xb[u], Db[u], k)
                gather(Sp, Xb[1 - u], jnp.minimum(k + 1, NB - 1))
                if Sn is not None:
                    act(Sn, k)
        point(Db[1], NB - 1)

    @pl.when(b == 0)
    def _():
        borders(S0)

        @loop(NB)
        def _(k):
            act(S0, k)

    inner = (b > 0) & (b < B)

    @pl.when(inner & (b % 2 == 0))
    def _():
        step(S0, S1)

    @pl.when(inner & (b % 2 == 1))
    def _():
        step(S1, S0)

    @pl.when(b == B)
    def _():
        step(None, S1)

    @pl.when(b > 0)
    def _():
        h_ref[0, 0] = hmax(PV, o_ref[0, 0], W)

        @loop(RC, unroll=2)
        def _(r):
            rn = jnp.minimum(2 * r + 2, R - 1)
            d_ref[0, r] = hmax(PV, jnp.maximum(jnp.maximum(o_ref[0, 2 * r], o_ref[0, 2 * r + 1]), o_ref[0, rn]), W)


def call_fine(two, three, p, ph, t, wts):
    def block(s, late=False):
        return pl.BlockSpec((1,) + s[1:], lambda b: (jnp.maximum(b - 1, 0) if late else jnp.minimum(b, B - 1), 0, 0, 0))
    full = [pl.BlockSpec(a.shape, lambda b, n=a.ndim: (0,) * n) for a in wts]
    outs = [shape(3, R3), shape(4, RC3), shape(4, 1)]
    S = vm((1, 2, R3 + 2, W3 + 2 * TILE, H), f32)
    X = vm((2, PB * W3 + TILE, K3))
    D = vm((2 * PB * W3 + TILE, C))
    return pl.pallas_call(
        fine, grid=(B + 1,),
        out_shape=[struct(s) for s in outs],
        in_specs=[SMEM] * 2 + [block(a.shape) for a in (p, ph, t)] + full,
        out_specs=[block(s, True) for s in outs],
        scratch_shapes=[S, S, vm((2, 2, W3, H), f32), X, X, D, D, vm((2, W3 + TILE, H), f32), vm((2, K3, C)), vm((9, TILE, C), f32)],
        compiler_params=pltpu.CompilerParams(vmem_limit_bytes=60 * MIB),
    )(two, three, p, ph, t, *wts)


def bottom_up(*refs, n_dev):
    take = splitter(refs)
    two, three, p4 = take(3)
    Ph = {4: p4, **dict(zip(LOW, take(3)))}
    Xh, Th = dict(zip(LV, take(4))), dict(zip(TD, take(3)))
    d4, h4, dw_ref, pw_ref, sc_ref, bi_ref = take(6)
    Oh = dict(zip(LV, take(4)))
    Pv, Tv, Dv, Ov = dict(zip(LV, take(4))), dict(zip(TD, take(3))), dict(zip(LV, take(4))), dict(zip(LV, take(4)))
    UP, UR, DR, S = [dict(zip(LV, take(4))) for _ in range(4)]
    V = dict(zip(TD, take(3)))
    F = dict(zip(LOW, take(3)))
    D, DW, ls, os, s_up, r_up, s_dn, r_dn = take(8)
    me = lax.axis_index('sp')
    last = n_dev - 1
    wts = (DW, pw_ref, sc_ref, bi_ref)

    def sl(g):
        return pl.ds(g * N, N)

    def loads(l, g):
        q = sl(g)
        pairs = [(Xh[l].at[q], Pv[l].at[q, pl.ds(0, 1)])]
        if l == TOP:
            pairs += [(p4.at[q], Pv[4].at[q, pl.ds(1, ROWS[4])]), (d4.at[q], Dv[4].at[q]), (h4.at[q], UP[4].at[q, pl.ds(0, 1)])]
        if l < END:
            pairs += [(Th[l].at[q], Tv[l].at[q])]
        return [pltpu.make_async_copy(a, b, ls.at[l - TOP, g, i]) for i, (a, b) in enumerate(pairs)]

    def up(l, g):
        return remote(UP[l].at[sl(g)], UR[l].at[sl(g)], s_up.at[l - TOP, g], r_up.at[l - TOP, g], me - 1)

    def dn(l, g):
        return remote(Dv[l].at[sl(g), pl.ds(ROWS[l] - 1, 1)], DR[l].at[sl(g)], s_dn.at[l - TOP, g], r_dn.at[l - TOP, g], me + 1)

    def send(l, g):
        @pl.when(me > 0)
        def _():
            up(l, g).start()

        @pl.when(me < last)
        def _():
            dn(l, g).start()

    def arrive(l, g):
        @pl.when(me < last)
        def _():
            up(l, g).wait_recv()

        @pl.when(me > 0)
        def _():
            dn(l, g).wait_recv()

    CF = {l: coefs(two, three, l) for l in LV}

    def fuse(l, b, r, d):
        a = CF[l]
        h = Pv[l][b, r + 1].astype(f32) * a[0] + d.astype(f32) * a[-1]
        if l < END:
            h = h + Tv[l][b, r + 1].astype(f32) * a[1]
        return h

    def first(l, b):
        UP[l][b, 1] = swish(fuse(l, b, 0, Dv[l][b, 0])).astype(bf16)

    barrier_signal(me, last)

    @groups
    def _(g):
        for l in LV:
            for c in loads(l, g):
                c.start()
    widen(dw_ref, DW)
    for l in LV:
        zero_edges(S[l], COLS[l])
        if l < END:
            V[l][:, COLS[l]:COLS[l] + TILE, :] = jnp.full((2, TILE, H), NEG, f32)

    @pl.when(me == last)
    def _():
        for l in LV:
            UR[l][:, :1] = jnp.full(shape(l, 1), NEG, bf16)
            UR[l][:, 1:] = jnp.zeros(shape(l, 1), bf16)

    @pl.when(me == 0)
    def _():
        for l in LV:
            DR[l][...] = jnp.zeros(shape(l, 1), bf16)

    barrier_wait(me, last)

    @groups
    def _(g):
        for c in loads(4, g):
            c.wait()

        @loop(N)
        def _(i):
            first(4, g * N + i)
        send(4, g)

    for l in LOW:
        W, R, st = COLS[l], ROWS[l], COLS[l] + 1

        @loop(B // 2)
        def _(i):
            for d in TWO:
                b = 2 * i + d
                for w in range(W):
                    for c, v in enumerate(halves(Ph[l][b, w].astype(f32))):
                        F[l][d, c, pl.ds(w, R, stride=st), :] = v
                for r in range(R):
                    Pv[l][b, 1 + r] = join([F[l][d, c, r * st:r * st + W, :] for c in TWO]).astype(bf16)

    def node(l, g):
        W, R = COLS[l], ROWS[l]
        nb = SLOTS[l]

        def borders(b, ib):
            put_s(S[l], ib, 0, W, fuse(l, b, -1, jnp.maximum(DR[l][b, 0], UP[l][b, 0])))
            put_s(S[l], ib, R, W, fuse(l, b, R - 1, jnp.maximum(Dv[l][b, R - 1], UR[l][b, 0])))
            for c, v in enumerate(halves(UR[l][b, 1].astype(f32))):
                S[l][ib, c, R + 1, cols(W), :] = v

            @pl.when(me == 0)
            def _():
                S[l][ib, :, 0, cols(W), :] = jnp.zeros((2, W, H), f32)

        def pools(b):
            n = R // 2

            def row(r):
                return Ov[l][b, r]
            UP[l + 1][b, 0] = hmax(V[l], row(0), W)

            def pooled(r, inner):
                m = jnp.maximum(row(2 * r), row(2 * r + 1))
                if inner:
                    m = jnp.maximum(m, row(2 * r + 2))
                Dv[l + 1][b, r] = hmax(V[l], m, W)
            if l == TOP:
                @loop(n - 1)
                def _(r):
                    pooled(r, True)
            else:
                for r in range(n - 1):
                    pooled(r, True)
            pooled(n - 1, False)
            first(l + 1, b)

        @loop(N // nb)
        def _(i):
            b0 = g * N + i * nb
            for ib in range(nb):
                borders(b0 + ib, ib)

            def put(ib, o, v):
                Ov[l][b0 + ib, o] = v
            if l == TOP:
                @loop((R - 1) // 3)
                def _(r):
                    for y in THREE:
                        put_s(S[l], 0, 3 * r + y + 1, W, fuse(l, b0, 3 * r + y, Dv[l][b0, 3 * r + y]))

                @loop(R // 4)
                def _(q):
                    conv_rows(S[l], D, [(0, q * 4 + y) for y in range(4)], l, l, wts, put)
            else:
                for ib in range(nb):
                    for r in range(R - 1):
                        put_s(S[l], ib, r + 1, W, fuse(l, b0 + ib, r, Dv[l][b0 + ib, r]))
                conv_rows(S[l], D, [(ib, o) for ib in range(nb) for o in range(R)], l, l, wts, put)
            if l < END:
                for ib in range(nb):
                    pools(b0 + ib)

    def out(l, g):
        return pltpu.make_async_copy(Ov[l].at[sl(g)], Oh[l].at[sl(g)], os.at[l - TOP, g])

    @loop(G + 3)
    def _(t):
        for l in LV:
            g = t - (l - 4)

            @pl.when((g >= 0) & (g < G))
            def _(l=l, g=g):
                if l < END:
                    for c in loads(l + 1, g):
                        c.wait()
                arrive(l, g)
                node(l, g)
                if l < END:
                    send(l + 1, g)
                out(l, g).start()

    for cond, cp in ((me > 0, up), (me < last, dn)):
        @pl.when(cond)
        def _(cp=cp):
            @groups
            def _(g):
                for l in LV:
                    cp(l, g).wait_send()

    @groups
    def _(g):
        for l in LV:
            out(l, g).wait()


def call_bottom_up(n_dev, two, three, p4, qs, xs, ts, d4, h4, wts):
    scratch = [vm(shape(l, ROWS[l] + 1)) for l in LV] + [vm(shape(l, ROWS[l] + 2)) for l in TD]
    scratch += [vm(shape(l, ROWS[l])) for l in LV] * 2 + [vm(shape(l, 2)) for l in LV] * 2 + [vm(shape(l, 1)) for l in LV]
    scratch += [vm((SLOTS[l], 2, ROWS[l] + 2, PADC[l] + 2 * TILE, H), f32) for l in LV] + [vm((2, PADC[l] + TILE, H), f32) for l in TD]
    scratch += [vm((2, 2, TILE * -(-ROWS[l] * (COLS[l] + 1) // TILE), H), f32) for l in LOW]
    scratch += [vm((24 * 16 + TILE, C)), vm((9, TILE, C), f32), DMA((4, G, 5))] + [DMA((4, G))] * 5
    return pl.pallas_call(
        functools.partial(bottom_up, n_dev=n_dev),
        out_shape=[struct(shape(l, ROWS[l])) for l in LV],
        in_specs=[SMEM] * 2 + [ANY] + [VMEM] * 3 + [ANY] * 9 + [VMEM] * 4,
        out_specs=[ANY] * 4,
        scratch_shapes=scratch,
        compiler_params=pltpu.CompilerParams(collective_id=1, has_side_effects=True, vmem_limit_bytes=62 * MIB),
    )(two, three, p4, *qs, *xs, *ts, d4, h4, *wts)


def finish(i4, i5, i6, i7, o4, o5, o6, o7, buf, F5, F6, F7, si, so):
    def cin(g):
        return pltpu.make_async_copy(i4.at[pl.ds(g * N, N)], buf.at[pl.ds(g * N, N)], si.at[g])

    def cout(g):
        return pltpu.make_async_copy(buf.at[pl.ds(g * N, N)], o4.at[pl.ds(g * N, N)], so.at[g])

    for g in range(G):
        cin(g).start()
    for g, (l, src, dst, F) in enumerate(((6, i6, o6, F6), (7, i7, o7, F7), (5, i5, o5, F5))):
        W, R, st = COLS[l], ROWS[l], COLS[l] + 1

        @loop(B // 2)
        def _(i):
            for d in TWO:
                b = 2 * i + d
                for r in range(R):
                    for c, v in enumerate(halves(src[b, r].astype(f32))):
                        F[d, c, r * st:r * st + W, :] = v
                for w in range(W):
                    dst[b, w] = join([F[d, c, pl.ds(w, R, stride=st), :] for c in TWO]).astype(bf16)
        cin(g).wait()
        cout(g).start()
    cin(G - 1).wait()
    cout(G - 1).start()
    for g in range(G):
        cout(g).wait()


def call_finish(ins):
    return pl.pallas_call(
        finish,
        out_shape=[struct(shape(4, ROWS[4]))] + [struct(flipped(l)) for l in LOW],
        in_specs=[ANY] + [VMEM] * 3,
        out_specs=[ANY] + [VMEM] * 3,
        scratch_shapes=[vm(shape(4, ROWS[4]))] + [vm((2, 2, TILE * -(-ROWS[l] * (COLS[l] + 1) // TILE), H), f32) for l in LOW] + [DMA((G,))] * 2,
        compiler_params=pltpu.CompilerParams(vmem_limit_bytes=62 * MIB),
    )(*ins)


def flip(a):
    return jnp.swapaxes(a, 1, 2)


def solution(mesh):
    n_dev = mesh.shape['sp']

    def body(p3, p4, p5, p6, p7, fuse_two, fuse_three, dw_filter, pw_weight, bn_scale, bn_bias):
        two, three = fuse_two.T, fuse_three
        qs = [flip(a) for a in (p5, p6, p7)]
        wts = (jnp.transpose(dw_filter, (1, 2, 0, 3)), pw_weight, bn_scale, bn_bias)
        t4, t5, t6, h3, *xs = call_top_down(n_dev, two, three, p3, p4, qs, wts)
        out3, d4, h4 = call_fine(two, three, p3, h3, t4, wts)
        outs = call_bottom_up(n_dev, two, three, p4, qs, xs, (t4, t5, t6), d4, h4, wts)
        out4, *rest = call_finish(outs)
        return out3, out4, *[flip(a) for a in rest]

    band_spec = P('dp', 'sp')
    whole = P()
    return jax.shard_map(body, mesh=mesh, in_specs=(band_spec,) * 5 + (whole,) * 6, out_specs=(band_spec,) * 5, check_vma=False)
```

```python
import functools

import jax
import jax.numpy as jnp
from jax import lax
from jax.experimental import pallas as pl
from jax.experimental.pallas import tpu as pltpu
from jax.sharding import PartitionSpec as P

f32, bf16 = jnp.float32, jnp.bfloat16
FUSE_EPS = 1e-4
B, C, H = 16, 256, 128
G, N = 4, 4
LV = (4, 5, 6, 7)
LOW = LV[1:]
TOP, END = 4, 7
TWO, THREE = range(2), range(3)
ROW0, ROW1 = pl.ds(0, 1), pl.ds(1, 1)
ROWS = {3: 32, 4: 16, 5: 8, 6: 4, 7: 2}
COLS = {3: 80, 4: 40, 5: 20, 6: 10, 7: 5}
PADC = {3: 80, 4: 40, 5: 24, 6: 16, 7: 8}
TILE = CHUNKS = 8
TWO_N = B // CHUNKS
MESH = pl.DeviceIdType.MESH
NEG = -jnp.inf
MIB = 2 ** 20


def groups(fn):
    def body(g, _):
        fn(g)
        return g
    lax.fori_loop(0, G, body, G)


def prev(t):
    return jnp.maximum(t - 1, 0)


def loop(n, unroll=1):
    def run(fn):
        def body(i, _):
            fn(i)
            return i
        lax.fori_loop(0, n, body, n, unroll=unroll)
    return run


def swish(h):
    return h + h * jnp.tanh(h)


def halves(v):
    return v[:, :H], v[:, H:]


def join(v):
    return jnp.concatenate(v, axis=1)


def half(c):
    return slice(c * H, c * H + H)


def cols(W, d=0):
    return slice(TILE + d, TILE + d + W)


def coefs(two, three, k):
    w = [two[i, min(k, 4)] for i in TWO] if k < 4 or k == 7 else [three[k - 4, i] for i in THREE]
    w = [jnp.maximum(x, 0.0) for x in w]
    total = jnp.full((1, C), sum(w[1:], w[0]) + FUSE_EPS, f32)
    return [jnp.full((1, C), 0.5 * x, f32) / total for x in w]


def widen(dw_ref, DW):
    for ky in THREE:
        for kx in THREE:
            DW[3 * ky + kx] = dw_ref[ky, kx].astype(f32)


def tap(DW, k, ky, kx, c):
    return DW[3 * ky + kx, k:k + 1, half(c)]


def zero_edges(S, W):
    S[..., :TILE, :] = jnp.zeros(S.shape[:-2] + (TILE, H), f32)
    S[..., TILE + W:, :] = jnp.zeros(S.shape[:-2] + (S.shape[-2] - TILE - W, H), f32)


def expand(U, v, wc):
    for c, h in enumerate(halves(v)):
        for d in TWO:
            U[c, pl.ds(d, wc, stride=2), :] = h
    return join([U[0], U[1]])


def put_s(S, ib, s, W, h):
    v = swish(h).astype(bf16).astype(f32)
    for c, x in enumerate(halves(v)):
        S[ib, c, s, cols(W), :] = x


def conv_row(S, ib, o, W, DW, k):
    out = []
    for c in TWO:
        acc = None
        for ky in THREE:
            for kx in THREE:
                t = S[ib, c, o + ky, cols(W, kx - 1), :] * tap(DW, k, ky, kx, c)
                acc = t if acc is None else acc + t
        out.append(acc)
    return join(out).astype(bf16)


def lagged(level, k, n, nq, step, S, D, wts, before, put, after):
    DW, pw_ref, sc_ref, bi_ref = wts
    W, wp = COLS[level], PADC[level]
    rows = [(ib, y) for ib in range(S.shape[0]) for y in range(step)]
    m = len(rows) * wp

    def point(t):
        i, q = t // nq, t % nq
        r = jnp.dot(D[t % 2, :m], pw_ref[k], preferred_element_type=f32)
        r = (r * sc_ref[k:k + 1] + bi_ref[k:k + 1]).astype(bf16)
        for x, (ib, y) in enumerate(rows):
            put(i, ib, q * step + y, r[x * wp:x * wp + W])

    def chunk(i, q):
        t = i * nq + q
        point(prev(t))
        for x, (ib, y) in enumerate(rows):
            D[t % 2, x * wp:x * wp + W, :] = conv_row(S, ib, q * step + y, W, DW, k)

    @loop(n)
    def _(i):
        before(i)
        if nq == 1:
            chunk(i, 0)
        else:
            @loop(nq)
            def _(q):
                chunk(i, q)
        if after is not None:
            @pl.when(i > 0)
            def _():
                after(i - 1)
    point(n * nq - 1)
    if after is not None:
        after(n - 1)


def hmax(PV, v, W):
    out = []
    for c, x in enumerate(halves(v.astype(f32))):
        PV[c, :W, :] = x
        a, b, d = [PV[c, pl.ds(i, W // 2, stride=2), :] for i in THREE]
        out.append(jnp.maximum(jnp.maximum(a, b), d))
    return join(out).astype(bf16)


def links(me, last, relay):
    lo, hi = last // 2, last // 2 + 1
    pairs = [(me > 0, me - 1), (me < last, me + 1)]
    if relay:
        for a, b in ((lo, last), (last, hi), (hi, 0), (0, lo)):
            pairs += [(me == a, b), (me == b, a)]
    return pairs


def images(fn):
    @loop(B // len(TWO))
    def _(i):
        for d in TWO:
            fn(len(TWO) * i + d, d)


def rows_first(l, src, dst, off, F):
    W, R, st = COLS[l], ROWS[l], COLS[l] + 1

    @images
    def _(b, d):
        for w in range(W):
            for c, v in enumerate(halves(src[b, w].astype(f32))):
                F[d, c, pl.ds(w, R, stride=st), :] = v
        for r in range(R):
            dst[b, off + r] = join([F[d, c, r * st:r * st + W, :] for c in TWO]).astype(bf16)


def barrier_signal(me, last, relay=False):
    sem = pltpu.get_barrier_semaphore()
    for cond, peer in links(me, last, relay):
        @pl.when(cond)
        def _(peer=peer):
            pl.semaphore_signal(sem, inc=1, device_id={'sp': peer}, device_id_type=MESH)


def barrier_wait(me, last, relay=False):
    sem = pltpu.get_barrier_semaphore()
    for d in range(last + 1):
        @pl.when(me == d)
        def _(d=d):
            pl.semaphore_wait(sem, sum(bool(c) for c, _ in links(d, last, relay)))


def remote(src, dst, ss, rs, dev):
    return pltpu.make_async_remote_copy(src_ref=src, dst_ref=dst, send_sem=ss, recv_sem=rs, device_id={'sp': dev}, device_id_type=MESH)


def shape(l, r):
    return (B, r, COLS[l], C)


def flipped(l):
    return (B, COLS[l], ROWS[l], C)


def vm(s, t=bf16):
    return pltpu.VMEM(s, t)


def flip_buffer(l):
    return vm((2, 2, TILE * -(-ROWS[l] * (COLS[l] + 1) // TILE), H), f32)


DMA = pltpu.SemaphoreType.DMA
ANY = pl.BlockSpec(memory_space=pl.ANY)
VMEM = pl.BlockSpec(memory_space=pltpu.VMEM)
SMEM = pl.BlockSpec(memory_space=pltpu.SMEM)


def struct(s):
    return jax.ShapeDtypeStruct(s, bf16)


def splitter(refs):
    it = iter(refs)

    def take(n):
        return [next(it) for _ in range(n)]
    return take


EXT = {4: 2, 5: 2, 6: 2, 7: 1}
TD = (4, 5, 6)
SLOTS = {4: 1, 5: 1, 6: N, 7: N}


def top_down(*refs, n_dev):
    take = splitter(refs)
    two, three, p3, p4 = take(4)
    Q = dict(zip(LOW, take(3)))
    dw_ref, pw_ref, sc_ref, bi_ref = take(4)
    Th = dict(zip(TD, take(3)))
    h3, = take(1)
    X = dict(zip(LV, take(4)))
    E, T = dict(zip(LV, take(4))), dict(zip(TD, take(3)))
    S, U, F = dict(zip(TD, take(3))), dict(zip(TD, take(3))), dict(zip(LOW, take(3)))
    D, Z, RB, DW, ls, os, xs, s_up, r_up, s_dn, r_dn, s3, r3, zs, rr, fs = take(16)
    lo, hi = (n_dev - 1) // 2, n_dev // 2
    me = lax.axis_index('sp')
    last = n_dev - 1
    wts = (DW, pw_ref, sc_ref, bi_ref)
    FINE_FIRST = (7, 6, 5, 4)

    def sl(g):
        return pl.ds(g * N, N)

    def load(g):
        return pltpu.make_async_copy(p4.at[sl(g)], E[4].at[sl(g), pl.ds(EXT[4], ROWS[4])], ls.at[g])

    def src(l, g, r):
        return p4.at[sl(g), pl.ds(r, EXT[l])] if l == TOP else E[l].at[sl(g), pl.ds(EXT[l] + r, EXT[l])]

    def up(l, g):
        e = EXT[l]
        return remote(src(l, g, 0), E[l].at[sl(g), pl.ds(e + ROWS[l], e)], s_up.at[l - TOP, g], r_up.at[l - TOP, g], me - 1)

    def dn(l, g):
        e = EXT[l]
        return remote(src(l, g, ROWS[l] - e), E[l].at[sl(g), pl.ds(0, e)], s_dn.at[l - TOP, g], r_dn.at[l - TOP, g], me + 1)

    up3 = remote(p3.at[:, ROW0], h3.at[:, ROW1], s3.at[0], r3.at[0], me - 1)
    dn3 = remote(p3.at[:, pl.ds(ROWS[3] - 1, 1)], h3.at[:, ROW0], s3.at[1], r3.at[1], me + 1)

    to_relay = {lo: remote(dn3.src_ref, RB, s3.at[1], rr, last), hi: remote(up3.src_ref, RB, s3.at[0], rr, 0)}
    from_relay = {0: remote(RB, h3.at[:, ROW1], fs, r3.at[0], lo), last: remote(RB, h3.at[:, ROW0], fs, r3.at[1], hi)}
    barrier_signal(me, last, True)

    @groups
    def _(g):
        load(g).start()

    barrier_wait(me, last, True)
    for d, cp in to_relay.items():
        @pl.when(me == d)
        def _(cp=cp):
            cp.start()

    for l in FINE_FIRST[:-1]:
        rows_first(l, Q[l], E[l], EXT[l], F[l])
    Z[...] = jnp.zeros(Z.shape, bf16)
    edge = [pltpu.make_async_copy(Z, h3.at[:, pl.ds(i, 1)], zs) for i in TWO]

    @pl.when(me == 0)
    def _():
        edge[0].start()
        for l in LV:
            E[l][:, :EXT[l]] = jnp.zeros(shape(l, EXT[l]), bf16)

    @pl.when(me == last)
    def _():
        edge[1].start()
        for l in LV:
            E[l][:, EXT[l] + ROWS[l]:] = jnp.zeros(shape(l, EXT[l]), bf16)

    for cond, cp, big, other in ((me > 0, up, up3, hi), (me < last, dn, dn3, lo)):
        @pl.when(cond)
        def _(cp=cp, big=big, other=other):
            @groups
            def _(g):
                for l in FINE_FIRST:
                    cp(l, g).start()

            @pl.when(me != other)
            def _():
                big.start()
    widen(dw_ref, DW)
    for l in TD:
        zero_edges(S[l], COLS[l])

    def node(l, g):
        k = 6 - l
        W, wc, R = COLS[l], COLS[l + 1], ROWS[l]
        a1, a2 = coefs(two, three, k)
        coarse = E[7] if l == 6 else T[l + 1]
        nb = SLOTS[l]

        def fill(b, ib, j, u):
            x = expand(U[l].at[u], coarse[b, j].astype(f32) * a2, wc)
            for d in TWO:
                put_s(S[l], ib, 2 * j + d, W, E[l][b, 2 * j + d].astype(f32) * a1 + x)

        def before(i):
            b0 = g * N + i * nb
            if l == TOP:
                @loop((R + 4) // 4)
                def _(j):
                    for u in TWO:
                        fill(b0, 0, 2 * j + u, u)
            else:
                for ib in range(nb):
                    for j in range((R + 4) // 2):
                        fill(b0 + ib, ib, j, (ib + j) % 2)

        def put(i, ib, o, v):
            T[l][g * N + i * nb + ib, o] = v
        nq = 3 if l == TOP else 1
        lagged(l, k, N // nb, nq, (R + 2) // nq, S[l], D, wts, before, put, None)

        for cond, o in ((me == 0, 0), (me == last, R + 1)):
            @pl.when(cond)
            def _(o=o):
                T[l][sl(g), o:o + 1] = jnp.zeros((N, 1, W, C), bf16)

    def out(l, g):
        return pltpu.make_async_copy(T[l].at[sl(g)], Th[l].at[sl(g)], os.at[l - TOP, g])

    def xout(l):
        return pltpu.make_async_copy(E[l].at[:, pl.ds(EXT[l] - 1, 1)], X[l], xs.at[l - 4])

    def arrive(l, g):
        @pl.when(me > 0)
        def _():
            dn(l, g).wait_recv()

        @pl.when(me < last)
        def _():
            up(l, g).wait_recv()

    @groups
    def _(g):
        arrive(7, g)
        for l in (6, 5, 4):
            if l == TOP:
                load(g).wait()
            arrive(l, g)
            node(l, g)
            out(l, g).start()
        for d, cp in from_relay.items():
            @pl.when((me == d) & (g == 0))
            def _(d=d, cp=cp):
                to_relay[hi if d == 0 else lo].wait_recv()
                cp.start()
    for l in LV:
        xout(l).start()
    for d, cp in from_relay.items():
        @pl.when(me == d)
        def _(cp=cp):
            cp.wait_send()

    for cond, cp, sent, got in ((me > 0, up, up3, dn3), (me < last, dn, dn3, up3)):
        @pl.when(cond)
        def _(cp=cp, sent=sent, got=got):
            @groups
            def _(g):
                for l in LV:
                    cp(l, g).wait_send()
            sent.wait_send()
            got.wait_recv()

    for cond, e in ((me == 0, edge[0]), (me == last, edge[1])):
        @pl.when(cond)
        def _(e=e):
            e.wait()
    for l in LV:
        xout(l).wait()

    @groups
    def _(g):
        for l in TD:
            out(l, g).wait()


def call_top_down(n_dev, two, three, p3, p4, qs, wts):
    scratch = [vm(shape(l, ROWS[l] + 2 * EXT[l])) for l in LV] + [vm(shape(l, ROWS[l] + 2)) for l in TD]
    scratch += [vm((SLOTS[l], 2, ROWS[l] + 4, PADC[l] + 2 * TILE, H), f32) for l in TD]
    scratch += [vm((2, 2, COLS[l], H), f32) for l in TD]
    scratch += [flip_buffer(l) for l in LOW]
    scratch += [vm((2, 24 * 16 + TILE, C)), vm(shape(3, 1)), vm(shape(3, 1)), vm((9, TILE, C), f32)]
    scratch += [DMA((G,)), DMA((3, G)), DMA((4,))] + [DMA((4, G))] * 4 + [DMA((2,))] * 2 + [DMA] * 3
    return pl.pallas_call(
        functools.partial(top_down, n_dev=n_dev),
        out_shape=[struct(shape(l, ROWS[l] + 2)) for l in TD] + [struct(shape(3, 2))] + [struct(shape(l, 1)) for l in LV],
        in_specs=[SMEM] * 2 + [ANY] * 2 + [VMEM] * 7,
        out_specs=[ANY] * 8,
        scratch_shapes=scratch,
        compiler_params=pltpu.CompilerParams(collective_id=0, has_side_effects=True, vmem_limit_bytes=60 * MIB),
    )(two, three, p3, p4, *qs, *wts)


R3, W3 = ROWS[3], COLS[3]
RC3, WC3 = ROWS[4], COLS[4]
PB = 4
NB = RC3 // PB
K3 = 3 * C


def fine(two, three, p_ref, ph_ref, t_ref, p4_ref, t4_ref, dw_ref, pw_ref, sc_ref, bi_ref, o_ref, d_ref, h_ref, S0, S1, U, X0, X1, D0, D1, PV, WD, DW):
    R, W, RC, WC = R3, W3, RC3, WC3
    Xb, Db = (X0, X1), (D0, D1)
    a1, a2 = coefs(two, three, 3)
    b = pl.program_id(0)

    @pl.when(b == 0)
    def _():
        widen(dw_ref, DW)
        zero_edges(S0, W)
        zero_edges(S1, W)
        PV[:, W:, :] = jnp.full((2, TILE, H), NEG, f32)
        eye = lax.broadcasted_iota(jnp.int32, (H, H), 0) == lax.broadcasted_iota(jnp.int32, (H, H), 1)
        for c in TWO:
            for kx in THREE:
                for pi in TWO:
                    for po in TWO:
                        v = jnp.where(eye, tap(DW, 3, 1 + pi - po, kx, c), 0.0)
                        r0 = kx * C + pi * H
                        WD[c, r0:r0 + H, half(po)] = v.astype(bf16)

    def p1(S, tj, rows, u):
        x = expand(U.at[u], t_ref[tj + 1].astype(f32) * a2, WC)
        for v, si in rows:
            put_s(S, 0, si, W, v.astype(f32) * a1 + x)

    def borders(S):
        p1(S, -1, [(ph_ref[0], 0)], 0)
        p1(S, RC, [(ph_ref[1], R + 1)], 1)

    def act(S, k):
        for t in range(PB):
            tj = k * PB + t
            p1(S, tj, [(p_ref[2 * tj + d], 2 * tj + d + 1) for d in TWO], t % 2)

    def gather(S, X, k):
        for c in TWO:
            for p in range(PB):
                for kx in THREE:
                    X[c, p * W:(p + 1) * W, kx * C:kx * C + C] = join(
                        [S[0, c, 2 * (k * PB + p) + 1 + par, cols(W, kx - 1), :] for par in TWO]).astype(bf16)

    def conv(S, X, D, k):
        for c in TWO:
            r = jnp.dot(X[c, :PB * W], WD[c], preferred_element_type=f32)
            for p in range(PB):
                for par in TWO:
                    si = 2 * (k * PB + p) + 3 * par
                    q = r[p * W:(p + 1) * W, half(par)]
                    for kx in THREE:
                        q = q + S[0, c, si, cols(W, kx - 1), :] * tap(DW, 3, 2 * par, kx, c)
                    y = 2 * p + par
                    D[y * W:(y + 1) * W, half(c)] = q.astype(bf16)

    def point(D, k):
        o = jnp.dot(D[:2 * PB * W], pw_ref[3], preferred_element_type=f32)
        o = (o * sc_ref[3:4] + bi_ref[3:4]).astype(bf16)
        for y in range(2 * PB):
            o_ref[2 * PB * k + y] = o[y * W:(y + 1) * W]

    def step(Sn, Sp):
        if Sn is not None:
            borders(Sn)
        gather(Sp, Xb[0], 0)

        @loop(NB // 2)
        def _(kk):
            for u in TWO:
                k = 2 * kk + u
                point(Db[1 - u], prev(k))
                conv(Sp, Xb[u], Db[u], k)
                gather(Sp, Xb[1 - u], jnp.minimum(k + 1, NB - 1))
                if Sn is not None:
                    act(Sn, k)
        point(Db[1], NB - 1)

    @pl.when(b == 0)
    def _():
        borders(S0)

        @loop(NB)
        def _(k):
            act(S0, k)

    inner = (b > 0) & (b < B)

    @pl.when(inner & (b % 2 == 0))
    def _():
        step(S0, S1)

    @pl.when(inner & (b % 2 == 1))
    def _():
        step(S1, S0)

    @pl.when(b == B)
    def _():
        step(None, S1)

    @pl.when(b > 0)
    def _():
        h_ref[0] = hmax(PV, o_ref[0], W)

        @loop(RC, unroll=2)
        def _(r):
            rn = jnp.minimum(2 * r + 2, R - 1)
            d_ref[r] = hmax(PV, jnp.maximum(jnp.maximum(o_ref[2 * r], o_ref[2 * r + 1]), o_ref[rn]), W)
        a = coefs(two, three, TOP)
        maps = (p4_ref[0], t4_ref[0], d_ref[0])
        h_ref[1] = swish(sum(x.astype(f32) * y for x, y in zip(maps, a))).astype(bf16)


def call_fine(two, three, p, ph, t, p4, wts):
    def block(s, late=False, row=0):
        return pl.BlockSpec((None,) + s[1:], lambda b: (prev(b) if late else jnp.minimum(b, B - 1), row, 0, 0))
    full = [pl.BlockSpec(a.shape, lambda b, n=a.ndim: (0,) * n) for a in wts]
    outs = [shape(3, R3), shape(4, RC3), shape(4, 2)]
    S = vm((1, 2, R3 + 2, W3 + 2 * TILE, H), f32)
    X = vm((2, PB * W3 + TILE, K3))
    D = vm((2 * PB * W3 + TILE, C))
    return pl.pallas_call(
        fine, grid=(B + 1,),
        out_shape=[struct(s) for s in outs],
        in_specs=[SMEM] * 2 + [block(a.shape) for a in (p, ph, t)] + [block(shape(4, 1), True, r) for r in TWO] + full,
        out_specs=[block(s, True) for s in outs],
        scratch_shapes=[S, S, vm((2, 2, W3, H), f32), X, X, D, D, vm((2, W3 + TILE, H), f32), vm((2, K3, C)), vm((9, TILE, C), f32)],
        compiler_params=pltpu.CompilerParams(vmem_limit_bytes=60 * MIB),
    )(two, three, p, ph, t, p4, t, *wts)


def bottom_up(*refs, n_dev):
    take = splitter(refs)
    two, three, p4 = take(3)
    Ph = {4: p4, **dict(zip(LOW, take(3)))}
    Xh, Th = dict(zip(LV, take(4))), dict(zip(TD, take(3)))
    d4, h4, dw_ref, pw_ref, sc_ref, bi_ref = take(6)
    Oh = dict(zip(LV, take(4)))
    Pv, Tv, Dv, Ov = dict(zip(LV, take(4))), dict(zip(TD, take(3))), dict(zip(LV, take(4))), dict(zip(LV, take(4)))
    UP, UR, DR, S = [dict(zip(LV, take(4))) for _ in range(4)]
    V = dict(zip(TD, take(3)))
    F = dict(zip(LOW, take(3)))
    D, DW, ls, os, s_up, r_up, s_dn, r_dn = take(8)
    me = lax.axis_index('sp')
    last = n_dev - 1
    wts = (DW, pw_ref, sc_ref, bi_ref)

    def sl(g):
        return pl.ds(g * N, N)

    def loads(l, g):
        q = sl(g)
        pairs = [(Xh[l].at[q], Pv[l].at[q, ROW0])]
        if l == TOP:
            pairs += [(p4.at[q], Pv[4].at[q, pl.ds(1, ROWS[4])]), (d4.at[q], Dv[4].at[q]), (h4.at[q], UP[4].at[q])]
        if l < END:
            pairs += [(Th[l].at[q], Tv[l].at[q])]
        return [pltpu.make_async_copy(a, b, ls.at[l - TOP, g, i]) for i, (a, b) in enumerate(pairs)]

    def up(l, g):
        return remote((h4 if l == TOP else UP[l]).at[sl(g)], UR[l].at[sl(g)], s_up.at[l - TOP, g], r_up.at[l - TOP, g], me - 1)

    def dn(l, g):
        return remote((d4 if l == TOP else Dv[l]).at[sl(g), pl.ds(ROWS[l] - 1, 1)], DR[l].at[sl(g)], s_dn.at[l - TOP, g], r_dn.at[l - TOP, g], me + 1)

    def send(l, g):
        @pl.when(me > 0)
        def _():
            up(l, g).start()

        @pl.when(me < last)
        def _():
            dn(l, g).start()

    def arrive(l, g):
        @pl.when(me < last)
        def _():
            up(l, g).wait_recv()

        @pl.when(me > 0)
        def _():
            dn(l, g).wait_recv()

    CF = {l: coefs(two, three, l) for l in LV}

    def fuse(l, b, r, d):
        a = CF[l]
        h = Pv[l][b, r + 1].astype(f32) * a[0] + d.astype(f32) * a[-1]
        if l < END:
            h = h + Tv[l][b, r + 1].astype(f32) * a[1]
        return h

    def first(l, b):
        UP[l][b, 1] = swish(fuse(l, b, 0, Dv[l][b, 0])).astype(bf16)

    barrier_signal(me, last)

    @groups
    def _(g):
        for l in LV:
            for c in loads(l, g):
                c.start()
    barrier_wait(me, last)

    @groups
    def _(g):
        send(4, g)
    widen(dw_ref, DW)
    for l in LV:
        zero_edges(S[l], COLS[l])
        if l < END:
            V[l][:, COLS[l]:COLS[l] + TILE, :] = jnp.full((2, TILE, H), NEG, f32)

    @pl.when(me == last)
    def _():
        for l in LV:
            UR[l][:, :1] = jnp.full(shape(l, 1), NEG, bf16)
            UR[l][:, 1:] = jnp.zeros(shape(l, 1), bf16)

    @pl.when(me == 0)
    def _():
        for l in LV:
            DR[l][...] = jnp.zeros(shape(l, 1), bf16)

    for l in LOW:
        rows_first(l, Ph[l], Pv[l], 1, F[l])

    def node(l, g):
        W, R = COLS[l], ROWS[l]
        nb = SLOTS[l]

        def borders(b, ib):
            put_s(S[l], ib, 0, W, fuse(l, b, -1, jnp.maximum(DR[l][b, 0], UP[l][b, 0])))
            put_s(S[l], ib, R, W, fuse(l, b, R - 1, jnp.maximum(Dv[l][b, R - 1], UR[l][b, 0])))
            for c, v in enumerate(halves(UR[l][b, 1].astype(f32))):
                S[l][ib, c, R + 1, cols(W), :] = v

            @pl.when(me == 0)
            def _():
                S[l][ib, :, 0, cols(W), :] = jnp.zeros((2, W, H), f32)

        def pools(b):
            n = R // 2

            def row(r):
                return Ov[l][b, r]
            UP[l + 1][b, 0] = hmax(V[l], row(0), W)

            def pooled(r, inner):
                m = jnp.maximum(row(2 * r), row(2 * r + 1))
                if inner:
                    m = jnp.maximum(m, row(2 * r + 2))
                Dv[l + 1][b, r] = hmax(V[l], m, W)
            if l == TOP:
                @loop(n - 1)
                def _(r):
                    pooled(r, True)
            else:
                for r in range(n - 1):
                    pooled(r, True)
            pooled(n - 1, False)
            first(l + 1, b)

        def before(i):
            b0 = g * N + i * nb
            for ib in range(nb):
                borders(b0 + ib, ib)
            if l == TOP:
                @loop((R - 1) // 3)
                def _(r):
                    for y in THREE:
                        put_s(S[l], 0, 3 * r + y + 1, W, fuse(l, b0, 3 * r + y, Dv[l][b0, 3 * r + y]))
            else:
                for ib in range(nb):
                    for r in range(R - 1):
                        put_s(S[l], ib, r + 1, W, fuse(l, b0 + ib, r, Dv[l][b0 + ib, r]))

        def put(i, ib, o, v):
            Ov[l][g * N + i * nb + ib, o] = v

        def after(i):
            for ib in range(nb):
                pools(g * N + i * nb + ib)
        nq = 4 if l == TOP else 1
        lagged(l, l, N // nb, nq, R // nq, S[l], D, wts, before, put, after if l < END else None)

    def out(l, g):
        return pltpu.make_async_copy(Ov[l].at[sl(g)], Oh[l].at[sl(g)], os.at[l - TOP, g])

    @loop(G + 3)
    def _(t):
        for l in LV:
            g = t - (l - 4)

            @pl.when((g >= 0) & (g < G))
            def _(l=l, g=g):
                if l == TOP:
                    for c in loads(l, g):
                        c.wait()
                if l < END:
                    for c in loads(l + 1, g):
                        c.wait()
                arrive(l, g)
                node(l, g)
                if l < END:
                    send(l + 1, g)
                out(l, g).start()

    for cond, cp in ((me > 0, up), (me < last, dn)):
        @pl.when(cond)
        def _(cp=cp):
            @groups
            def _(g):
                for l in LV:
                    cp(l, g).wait_send()

    @groups
    def _(g):
        for l in LV:
            out(l, g).wait()


def call_bottom_up(n_dev, two, three, p4, qs, xs, ts, d4, h4, wts):
    scratch = [vm(shape(l, ROWS[l] + 1)) for l in LV] + [vm(shape(l, ROWS[l] + 2)) for l in TD]
    scratch += [vm(shape(l, ROWS[l])) for l in LV] * 2 + [vm(shape(l, 2)) for l in LV] * 2 + [vm(shape(l, 1)) for l in LV]
    scratch += [vm((SLOTS[l], 2, ROWS[l] + 2, PADC[l] + 2 * TILE, H), f32) for l in LV] + [vm((2, PADC[l] + TILE, H), f32) for l in TD]
    scratch += [flip_buffer(l) for l in LOW]
    scratch += [vm((2, 24 * 16 + TILE, C)), vm((9, TILE, C), f32), DMA((4, G, 5))] + [DMA((4, G))] * 5
    return pl.pallas_call(
        functools.partial(bottom_up, n_dev=n_dev),
        out_shape=[struct(shape(l, ROWS[l])) for l in LV],
        in_specs=[SMEM] * 2 + [ANY] + [VMEM] * 3 + [ANY] * 9 + [VMEM] * 4,
        out_specs=[ANY] * 4,
        scratch_shapes=scratch,
        compiler_params=pltpu.CompilerParams(collective_id=1, has_side_effects=True, vmem_limit_bytes=62 * MIB),
    )(two, three, p4, *qs, *xs, *ts, d4, h4, *wts)


def finish(i4, i5, i6, i7, o4, o5, o6, o7, buf, F5, F6, F7, si, so):
    def cin(g):
        return pltpu.make_async_copy(i4.at[pl.ds(TWO_N * g, TWO_N)], buf.at[pl.ds(TWO_N * g, TWO_N)], si.at[g])

    def cout(g):
        return pltpu.make_async_copy(buf.at[pl.ds(TWO_N * g, TWO_N)], o4.at[pl.ds(TWO_N * g, TWO_N)], so.at[g])

    @loop(CHUNKS)
    def _(g):
        cin(g).start()
    for l, src, dst, F in ((6, i6, o6, F6), (7, i7, o7, F7), (5, i5, o5, F5)):
        W, R, st = COLS[l], ROWS[l], COLS[l] + 1

        @loop(CHUNKS)
        def _(i):
            if l == 5:
                cin(i).wait()
                cout(i).start()
            for d in TWO:
                b = 2 * i + d
                for r in range(R):
                    for c, v in enumerate(halves(src[b, r].astype(f32))):
                        F[d, c, r * st:r * st + W, :] = v
                for w in range(W):
                    dst[b, w] = join([F[d, c, pl.ds(w, R, stride=st), :] for c in TWO]).astype(bf16)

    @loop(CHUNKS)
    def _(g):
        cout(g).wait()


def call_finish(ins):
    return pl.pallas_call(
        finish,
        out_shape=[struct(shape(4, ROWS[4]))] + [struct(flipped(l)) for l in LOW],
        in_specs=[ANY] + [VMEM] * 3,
        out_specs=[ANY] + [VMEM] * 3,
        scratch_shapes=[vm(shape(4, ROWS[4]))] + [flip_buffer(l) for l in LOW] + [DMA((CHUNKS,))] * 2,
        compiler_params=pltpu.CompilerParams(vmem_limit_bytes=62 * MIB),
    )(*ins)


def flip(a):
    return jnp.swapaxes(a, 1, 2)


def solution(mesh):
    n_dev = mesh.shape['sp']

    def body(p3, p4, p5, p6, p7, fuse_two, fuse_three, dw_filter, pw_weight, bn_scale, bn_bias):
        two, three = fuse_two.T, fuse_three
        qs = [flip(a) for a in (p5, p6, p7)]
        wts = (jnp.transpose(dw_filter, (1, 2, 0, 3)), pw_weight, bn_scale, bn_bias)
        t4, t5, t6, h3, *xs = call_top_down(n_dev, two, three, p3, p4, qs, wts)
        out3, d4, h4 = call_fine(two, three, p3, h3, t4, p4, wts)
        outs = call_bottom_up(n_dev, two, three, p4, qs, xs, (t4, t5, t6), d4, h4, wts)
        out4, *rest = call_finish(outs)
        return out3, out4, *[flip(a) for a in rest]

    band_spec = P('dp', 'sp')
    whole = P()
    return jax.shard_map(body, mesh=mesh, in_specs=(band_spec,) * 5 + (whole,) * 6, out_specs=(band_spec,) * 5, check_vma=False)
```

```python
import functools

import jax
import jax.numpy as jnp
from jax import lax
from jax.experimental import pallas as pl
from jax.experimental.pallas import tpu as pltpu
from jax.sharding import PartitionSpec as P

f32, bf16 = jnp.float32, jnp.bfloat16
FUSE_EPS = 1e-4
B, C, H = 16, 256, 128
G, N = 4, 4
LV = (4, 5, 6, 7)
LOW = LV[1:]
TOP, END = 4, 7
TWO, THREE = range(2), range(3)
ROW0, ROW1 = pl.ds(0, 1), pl.ds(1, 1)
ROWS = {3: 32, 4: 16, 5: 8, 6: 4, 7: 2}
COLS = {3: 80, 4: 40, 5: 20, 6: 10, 7: 5}
PADC = {3: 80, 4: 40, 5: 24, 6: 16, 7: 8}
TILE = CHUNKS = 8
TWO_N = B // CHUNKS
MESH = pl.DeviceIdType.MESH
NEG = -jnp.inf
MIB = 2 ** 20


def groups(fn):
    def body(g, _):
        fn(g)
        return g
    lax.fori_loop(0, G, body, G)


def prev(t):
    return jnp.maximum(t - 1, 0)


def loop(n, unroll=1):
    def run(fn):
        def body(i, _):
            fn(i)
            return i
        lax.fori_loop(0, n, body, n, unroll=unroll)
    return run


def swish(h):
    return h + h * jnp.tanh(h)


def halves(v):
    return v[:, :H], v[:, H:]


def join(v):
    return jnp.concatenate(v, axis=1)


def half(c):
    return slice(c * H, c * H + H)


def cols(W, d=0):
    return slice(TILE + d, TILE + d + W)


def coefs(two, three, k):
    w = [two[i, min(k, 4)] for i in TWO] if k < 4 or k == 7 else [three[k - 4, i] for i in THREE]
    w = [jnp.maximum(x, 0.0) for x in w]
    total = jnp.full((1, C), sum(w[1:], w[0]) + FUSE_EPS, f32)
    return [jnp.full((1, C), 0.5 * x, f32) / total for x in w]


def widen(dw_ref, DW):
    for ky in THREE:
        for kx in THREE:
            DW[3 * ky + kx] = dw_ref[ky, kx].astype(f32)


def tap(DW, k, ky, kx, c):
    return DW[3 * ky + kx, k:k + 1, half(c)]


def zero_edges(S, W):
    S[..., :TILE, :] = jnp.zeros(S.shape[:-2] + (TILE, H), f32)
    S[..., TILE + W:, :] = jnp.zeros(S.shape[:-2] + (S.shape[-2] - TILE - W, H), f32)


def expand(U, v, wc):
    for c, h in enumerate(halves(v)):
        for d in TWO:
            U[c, pl.ds(d, wc, stride=2), :] = h
    return join([U[0], U[1]])


def put_s(S, ib, s, W, h):
    v = swish(h).astype(bf16).astype(f32)
    for c, x in enumerate(halves(v)):
        S[ib, c, s, cols(W), :] = x


def conv_row(S, ib, o, W, DW, k):
    out = []
    for c in TWO:
        acc = None
        for ky in THREE:
            for kx in THREE:
                t = S[ib, c, o + ky, cols(W, kx - 1), :] * tap(DW, k, ky, kx, c)
                acc = t if acc is None else acc + t
        out.append(acc)
    return join(out).astype(bf16)


def lagged(level, k, n, nq, step, S, D, wts, before, put, after):
    DW, pw_ref, sc_ref, bi_ref = wts
    W, wp = COLS[level], PADC[level]
    rows = [(ib, y) for ib in range(S.shape[0]) for y in range(step)]
    m = len(rows) * wp

    def point(t):
        i, q = t // nq, t % nq
        r = jnp.dot(D[t % 2, :m], pw_ref[k], preferred_element_type=f32)
        r = (r * sc_ref[k:k + 1] + bi_ref[k:k + 1]).astype(bf16)
        for x, (ib, y) in enumerate(rows):
            put(i, ib, q * step + y, r[x * wp:x * wp + W])

    def chunk(i, q):
        t = i * nq + q
        point(prev(t))
        for x, (ib, y) in enumerate(rows):
            D[t % 2, x * wp:x * wp + W, :] = conv_row(S, ib, q * step + y, W, DW, k)

    @loop(n)
    def _(i):
        before(i)
        if nq == 1:
            chunk(i, 0)
        else:
            @loop(nq)
            def _(q):
                chunk(i, q)
        if after is not None:
            @pl.when(i > 0)
            def _():
                after(i - 1)
    point(n * nq - 1)
    if after is not None:
        after(n - 1)


def hmax(PV, v, W):
    out = []
    for c, x in enumerate(halves(v.astype(f32))):
        PV[c, :W, :] = x
        a, b, d = [PV[c, pl.ds(i, W // 2, stride=2), :] for i in THREE]
        out.append(jnp.maximum(jnp.maximum(a, b), d))
    return join(out).astype(bf16)


def links(me, last, relay):
    lo, hi = last // 2, last // 2 + 1
    pairs = [(me > 0, me - 1), (me < last, me + 1)]
    if relay:
        for a, b in ((lo, last), (last, hi), (hi, 0), (0, lo)):
            pairs += [(me == a, b), (me == b, a)]
    return pairs


def images(fn):
    @loop(B // len(TWO))
    def _(i):
        for d in TWO:
            fn(len(TWO) * i + d, d)


def rows_first(l, src, dst, off, F):
    W, R, st = COLS[l], ROWS[l], COLS[l] + 1

    @images
    def _(b, d):
        for w in range(W):
            for c, v in enumerate(halves(src[b, w].astype(f32))):
                F[d, c, pl.ds(w, R, stride=st), :] = v
        for r in range(R):
            dst[b, off + r] = join([F[d, c, r * st:r * st + W, :] for c in TWO]).astype(bf16)


def barrier_signal(me, last, relay=False):
    sem = pltpu.get_barrier_semaphore()
    for cond, peer in links(me, last, relay):
        @pl.when(cond)
        def _(peer=peer):
            pl.semaphore_signal(sem, inc=1, device_id={'sp': peer}, device_id_type=MESH)


def barrier_wait(me, last, relay=False):
    sem = pltpu.get_barrier_semaphore()
    for d in range(last + 1):
        @pl.when(me == d)
        def _(d=d):
            pl.semaphore_wait(sem, sum(bool(c) for c, _ in links(d, last, relay)))


def remote(src, dst, ss, rs, dev):
    return pltpu.make_async_remote_copy(src_ref=src, dst_ref=dst, send_sem=ss, recv_sem=rs, device_id={'sp': dev}, device_id_type=MESH)


def shape(l, r):
    return (B, r, COLS[l], C)


def flipped(l):
    return (B, COLS[l], ROWS[l], C)


def vm(s, t=bf16):
    return pltpu.VMEM(s, t)


def flip_buffer(l):
    return vm((2, 2, TILE * -(-ROWS[l] * (COLS[l] + 1) // TILE), H), f32)


DMA = pltpu.SemaphoreType.DMA
ANY = pl.BlockSpec(memory_space=pl.ANY)
VMEM = pl.BlockSpec(memory_space=pltpu.VMEM)
SMEM = pl.BlockSpec(memory_space=pltpu.SMEM)


def struct(s):
    return jax.ShapeDtypeStruct(s, bf16)


def splitter(refs):
    it = iter(refs)

    def take(n):
        return [next(it) for _ in range(n)]
    return take


EXT = {4: 2, 5: 2, 6: 2, 7: 1}
TD = (4, 5, 6)
SLOTS = {4: 1, 5: 1, 6: N, 7: N}


def top_down(*refs, n_dev):
    take = splitter(refs)
    two, three, p3, p4 = take(4)
    Q = dict(zip(LOW, take(3)))
    dw_ref, pw_ref, sc_ref, bi_ref = take(4)
    Th = dict(zip(TD, take(3)))
    h3, = take(1)
    X = dict(zip(LV, take(4)))
    E, T = dict(zip(LV, take(4))), dict(zip(TD, take(3)))
    S, U, F = dict(zip(TD, take(3))), dict(zip(TD, take(3))), dict(zip(LOW, take(3)))
    D, Z, RB, DW, ls, os, xs, s_up, r_up, s_dn, r_dn, s3, r3, zs, rr, fs = take(16)
    lo, hi = (n_dev - 1) // 2, n_dev // 2
    me = lax.axis_index('sp')
    last = n_dev - 1
    wts = (DW, pw_ref, sc_ref, bi_ref)
    FINE_FIRST = (7, 6, 5, 4)

    def sl(g):
        return pl.ds(g * N, N)

    def load(g):
        return pltpu.make_async_copy(p4.at[sl(g)], E[4].at[sl(g), pl.ds(EXT[4], ROWS[4])], ls.at[g])

    def src(l, g, r):
        return p4.at[sl(g), pl.ds(r, EXT[l])] if l == TOP else E[l].at[sl(g), pl.ds(EXT[l] + r, EXT[l])]

    def up(l, g):
        e = EXT[l]
        return remote(src(l, g, 0), E[l].at[sl(g), pl.ds(e + ROWS[l], e)], s_up.at[l - TOP, g], r_up.at[l - TOP, g], me - 1)

    def dn(l, g):
        e = EXT[l]
        return remote(src(l, g, ROWS[l] - e), E[l].at[sl(g), pl.ds(0, e)], s_dn.at[l - TOP, g], r_dn.at[l - TOP, g], me + 1)

    up3 = remote(p3.at[:, ROW0], h3.at[:, ROW1], s3.at[0], r3.at[0], me - 1)
    dn3 = remote(p3.at[:, pl.ds(ROWS[3] - 1, 1)], h3.at[:, ROW0], s3.at[1], r3.at[1], me + 1)

    to_relay = {lo: remote(dn3.src_ref, RB, s3.at[1], rr, last), hi: remote(up3.src_ref, RB, s3.at[0], rr, 0)}
    from_relay = {0: remote(RB, h3.at[:, ROW1], fs, r3.at[0], lo), last: remote(RB, h3.at[:, ROW0], fs, r3.at[1], hi)}
    barrier_signal(me, last, True)

    @groups
    def _(g):
        load(g).start()

    barrier_wait(me, last, True)
    for d, cp in to_relay.items():
        @pl.when(me == d)
        def _(cp=cp):
            cp.start()

    for l in FINE_FIRST[:-1]:
        rows_first(l, Q[l], E[l], EXT[l], F[l])
    Z[...] = jnp.zeros(Z.shape, bf16)
    edge = [pltpu.make_async_copy(Z, h3.at[:, pl.ds(i, 1)], zs) for i in TWO]

    @pl.when(me == 0)
    def _():
        edge[0].start()
        for l in LV:
            E[l][:, :EXT[l]] = jnp.zeros(shape(l, EXT[l]), bf16)

    @pl.when(me == last)
    def _():
        edge[1].start()
        for l in LV:
            E[l][:, EXT[l] + ROWS[l]:] = jnp.zeros(shape(l, EXT[l]), bf16)

    for cond, cp, big, other in ((me > 0, up, up3, hi), (me < last, dn, dn3, lo)):
        @pl.when(cond)
        def _(cp=cp, big=big, other=other):
            @groups
            def _(g):
                for l in FINE_FIRST:
                    cp(l, g).start()

            @pl.when(me != other)
            def _():
                big.start()
    widen(dw_ref, DW)
    for l in TD:
        zero_edges(S[l], COLS[l])

    def node(l, g):
        k = 6 - l
        W, wc, R = COLS[l], COLS[l + 1], ROWS[l]
        a1, a2 = coefs(two, three, k)
        coarse = E[7] if l == 6 else T[l + 1]
        nb = SLOTS[l]

        def fill(b, ib, j, u):
            x = expand(U[l].at[u], coarse[b, j].astype(f32) * a2, wc)
            for d in TWO:
                put_s(S[l], ib, 2 * j + d, W, E[l][b, 2 * j + d].astype(f32) * a1 + x)

        def before(i):
            b0 = g * N + i * nb
            if l == TOP:
                @loop((R + 4) // 4)
                def _(j):
                    for u in TWO:
                        fill(b0, 0, 2 * j + u, u)
            else:
                for ib in range(nb):
                    for j in range((R + 4) // 2):
                        fill(b0 + ib, ib, j, (ib + j) % 2)

        def put(i, ib, o, v):
            T[l][g * N + i * nb + ib, o] = v
        nq = 3 if l == TOP else 1
        lagged(l, k, N // nb, nq, (R + 2) // nq, S[l], D, wts, before, put, None)

        for cond, o in ((me == 0, 0), (me == last, R + 1)):
            @pl.when(cond)
            def _(o=o):
                T[l][sl(g), o:o + 1] = jnp.zeros((N, 1, W, C), bf16)

    def out(l, g):
        return pltpu.make_async_copy(T[l].at[sl(g)], Th[l].at[sl(g)], os.at[l - TOP, g])

    def xout(l):
        return pltpu.make_async_copy(E[l].at[:, pl.ds(EXT[l] - 1, 1)], X[l], xs.at[l - 4])

    def arrive(l, g):
        @pl.when(me > 0)
        def _():
            dn(l, g).wait_recv()

        @pl.when(me < last)
        def _():
            up(l, g).wait_recv()

    @groups
    def _(g):
        arrive(7, g)
        for l in (6, 5, 4):
            if l == TOP:
                load(g).wait()
            arrive(l, g)
            node(l, g)
            out(l, g).start()
        for d, cp in from_relay.items():
            @pl.when((me == d) & (g == 0))
            def _(d=d, cp=cp):
                to_relay[hi if d == 0 else lo].wait_recv()
                cp.start()
    for l in LV:
        xout(l).start()
    for d, cp in from_relay.items():
        @pl.when(me == d)
        def _(cp=cp):
            cp.wait_send()

    for cond, cp, sent, got in ((me > 0, up, up3, dn3), (me < last, dn, dn3, up3)):
        @pl.when(cond)
        def _(cp=cp, sent=sent, got=got):
            @groups
            def _(g):
                for l in LV:
                    cp(l, g).wait_send()
            sent.wait_send()
            got.wait_recv()

    for cond, e in ((me == 0, edge[0]), (me == last, edge[1])):
        @pl.when(cond)
        def _(e=e):
            e.wait()
    for l in LV:
        xout(l).wait()

    @groups
    def _(g):
        for l in TD:
            out(l, g).wait()


def call_top_down(n_dev, two, three, p3, p4, qs, wts):
    scratch = [vm(shape(l, ROWS[l] + 2 * EXT[l])) for l in LV] + [vm(shape(l, ROWS[l] + 2)) for l in TD]
    scratch += [vm((SLOTS[l], 2, ROWS[l] + 4, PADC[l] + 2 * TILE, H), f32) for l in TD]
    scratch += [vm((2, 2, COLS[l], H), f32) for l in TD]
    scratch += [flip_buffer(l) for l in LOW]
    scratch += [vm((2, 24 * 16 + TILE, C)), vm(shape(3, 1)), vm(shape(3, 1)), vm((9, TILE, C), f32)]
    scratch += [DMA((G,)), DMA((3, G)), DMA((4,))] + [DMA((4, G))] * 4 + [DMA((2,))] * 2 + [DMA] * 3
    return pl.pallas_call(
        functools.partial(top_down, n_dev=n_dev),
        out_shape=[struct(shape(l, ROWS[l] + 2)) for l in TD] + [struct(shape(3, 2))] + [struct(shape(l, 1)) for l in LV],
        in_specs=[SMEM] * 2 + [ANY] * 2 + [VMEM] * 7,
        out_specs=[ANY] * 8,
        scratch_shapes=scratch,
        compiler_params=pltpu.CompilerParams(collective_id=0, has_side_effects=True, vmem_limit_bytes=60 * MIB),
    )(two, three, p3, p4, *qs, *wts)


R3, W3 = ROWS[3], COLS[3]
RC3, WC3 = ROWS[4], COLS[4]
PB = 4
NB = RC3 // PB
K3 = 3 * C


def fine(two, three, p_ref, ph_ref, t_ref, p4_ref, t4_ref, dw_ref, pw_ref, sc_ref, bi_ref, o_ref, d_ref, h_ref, S0, S1, U, X0, X1, D0, D1, PV, WD, DW):
    R, W, RC, WC = R3, W3, RC3, WC3
    Xb, Db = (X0, X1), (D0, D1)
    a1, a2 = coefs(two, three, 3)
    b = pl.program_id(0)

    @pl.when(b == 0)
    def _():
        widen(dw_ref, DW)
        zero_edges(S0, W)
        zero_edges(S1, W)
        PV[..., W:, :] = jnp.full((PB, 2, TILE, H), NEG, f32)
        eye = lax.broadcasted_iota(jnp.int32, (H, H), 0) == lax.broadcasted_iota(jnp.int32, (H, H), 1)
        for c in TWO:
            for kx in THREE:
                for pi in TWO:
                    for po in TWO:
                        v = jnp.where(eye, tap(DW, 3, 1 + pi - po, kx, c), 0.0)
                        r0 = kx * C + pi * H
                        WD[c, r0:r0 + H, half(po)] = v.astype(bf16)

    def p1(S, tj, rows, u):
        x = expand(U.at[u], t_ref[tj + 1].astype(f32) * a2, WC)
        for v, si in rows:
            put_s(S, 0, si, W, v.astype(f32) * a1 + x)

    def borders(S):
        p1(S, -1, [(ph_ref[0], 0)], 0)
        p1(S, RC, [(ph_ref[1], R + 1)], 1)

    def act(S, k):
        for t in range(PB):
            tj = k * PB + t
            p1(S, tj, [(p_ref[2 * tj + d], 2 * tj + d + 1) for d in TWO], t % 2)

    def gather(S, X, k):
        for c in TWO:
            for p in range(PB):
                for kx in THREE:
                    X[c, p * W:(p + 1) * W, kx * C:kx * C + C] = join(
                        [S[0, c, 2 * (k * PB + p) + 1 + par, cols(W, kx - 1), :] for par in TWO]).astype(bf16)

    def conv(S, X, D, k):
        for c in TWO:
            r = jnp.dot(X[c, :PB * W], WD[c], preferred_element_type=f32)
            for p in range(PB):
                for par in TWO:
                    si = 2 * (k * PB + p) + 3 * par
                    q = r[p * W:(p + 1) * W, half(par)]
                    for kx in THREE:
                        q = q + S[0, c, si, cols(W, kx - 1), :] * tap(DW, 3, 2 * par, kx, c)
                    y = 2 * p + par
                    D[y * W:(y + 1) * W, half(c)] = q.astype(bf16)

    def point(D, k):
        o = jnp.dot(D[:2 * PB * W], pw_ref[3], preferred_element_type=f32)
        o = (o * sc_ref[3:4] + bi_ref[3:4]).astype(bf16)
        for y in range(2 * PB):
            o_ref[2 * PB * k + y] = o[y * W:(y + 1) * W]

    def step(Sn, Sp):
        if Sn is not None:
            borders(Sn)
        for k in range(NB):
            u = k % 2
            conv(Sp, Xb[u], Db[u], k)
            if k:
                point(Db[1 - u], k - 1)
            if k < NB - 1:
                gather(Sp, Xb[1 - u], k + 1)
            elif Sn is not None:
                gather(Sn, Xb[1 - u], 0)
            if Sn is not None:
                act(Sn, k)
        point(Db[1], NB - 1)

    @pl.when(b == 0)
    def _():
        borders(S0)

        @loop(NB)
        def _(k):
            act(S0, k)
        gather(S0, X0, 0)

    inner = (b > 0) & (b < B)

    @pl.when(inner & (b % 2 == 0))
    def _():
        step(S0, S1)

    @pl.when(inner & (b % 2 == 1))
    def _():
        step(S1, S0)

    @pl.when(b == B)
    def _():
        step(None, S1)

    @pl.when(b > 0)
    def _():
        h_ref[0] = hmax(PV.at[0], o_ref[0], W)

        @loop(RC // PB)
        def _(q):
            for y in range(PB):
                r = q * PB + y
                rn = jnp.minimum(2 * r + 2, R - 1)
                d_ref[r] = hmax(PV.at[y], jnp.maximum(jnp.maximum(o_ref[2 * r], o_ref[2 * r + 1]), o_ref[rn]), W)
        a = coefs(two, three, TOP)
        maps = (p4_ref[0], t4_ref[0], d_ref[0])
        h_ref[1] = swish(sum(x.astype(f32) * y for x, y in zip(maps, a))).astype(bf16)


def call_fine(two, three, p, ph, t, p4, wts):
    def block(s, late=False, row=0):
        return pl.BlockSpec((None,) + s[1:], lambda b: (prev(b) if late else jnp.minimum(b, B - 1), row, 0, 0))
    full = [pl.BlockSpec(a.shape, lambda b, n=a.ndim: (0,) * n) for a in wts]
    outs = [shape(3, R3), shape(4, RC3), shape(4, 2)]
    S = vm((1, 2, R3 + 2, W3 + 2 * TILE, H), f32)
    X = vm((2, PB * W3 + TILE, K3))
    D = vm((2 * PB * W3 + TILE, C))
    return pl.pallas_call(
        fine, grid=(B + 1,),
        out_shape=[struct(s) for s in outs],
        in_specs=[SMEM] * 2 + [block(a.shape) for a in (p, ph, t)] + [block(shape(4, 1), True, r) for r in TWO] + full,
        out_specs=[block(s, True) for s in outs],
        scratch_shapes=[S, S, vm((2, 2, W3, H), f32), X, X, D, D, vm((PB, 2, W3 + TILE, H), f32), vm((2, K3, C)), vm((9, TILE, C), f32)],
        compiler_params=pltpu.CompilerParams(vmem_limit_bytes=60 * MIB),
    )(two, three, p, ph, t, p4, t, *wts)


def bottom_up(*refs, n_dev):
    take = splitter(refs)
    two, three, p4 = take(3)
    Ph = {4: p4, **dict(zip(LOW, take(3)))}
    Xh, Th = dict(zip(LV, take(4))), dict(zip(TD, take(3)))
    d4, h4, dw_ref, pw_ref, sc_ref, bi_ref = take(6)
    Oh = dict(zip(LV, take(4)))
    Pv, Tv, Dv, Ov = dict(zip(LV, take(4))), dict(zip(TD, take(3))), dict(zip(LV, take(4))), dict(zip(LV, take(4)))
    UP, UR, DR, S = [dict(zip(LV, take(4))) for _ in range(4)]
    V = dict(zip(TD, take(3)))
    F = dict(zip(LOW, take(3)))
    D, DW, ls, os, s_up, r_up, s_dn, r_dn = take(8)
    me = lax.axis_index('sp')
    last = n_dev - 1
    wts = (DW, pw_ref, sc_ref, bi_ref)

    def sl(g):
        return pl.ds(g * N, N)

    def loads(l, g):
        q = sl(g)
        pairs = [(Xh[l].at[q], Pv[l].at[q, ROW0])]
        if l == TOP:
            pairs += [(p4.at[q], Pv[4].at[q, pl.ds(1, ROWS[4])]), (d4.at[q], Dv[4].at[q]), (h4.at[q], UP[4].at[q])]
        if l < END:
            pairs += [(Th[l].at[q], Tv[l].at[q])]
        return [pltpu.make_async_copy(a, b, ls.at[l - TOP, g, i]) for i, (a, b) in enumerate(pairs)]

    def up(l, g):
        return remote((h4 if l == TOP else UP[l]).at[sl(g)], UR[l].at[sl(g)], s_up.at[l - TOP, g], r_up.at[l - TOP, g], me - 1)

    def dn(l, g):
        return remote((d4 if l == TOP else Dv[l]).at[sl(g), pl.ds(ROWS[l] - 1, 1)], DR[l].at[sl(g)], s_dn.at[l - TOP, g], r_dn.at[l - TOP, g], me + 1)

    def send(l, g):
        @pl.when(me > 0)
        def _():
            up(l, g).start()

        @pl.when(me < last)
        def _():
            dn(l, g).start()

    def arrive(l, g):
        @pl.when(me < last)
        def _():
            up(l, g).wait_recv()

        @pl.when(me > 0)
        def _():
            dn(l, g).wait_recv()

    CF = {l: coefs(two, three, l) for l in LV}

    def fuse(l, b, r, d):
        a = CF[l]
        h = Pv[l][b, r + 1].astype(f32) * a[0] + d.astype(f32) * a[-1]
        if l < END:
            h = h + Tv[l][b, r + 1].astype(f32) * a[1]
        return h

    def first(l, b):
        UP[l][b, 1] = swish(fuse(l, b, 0, Dv[l][b, 0])).astype(bf16)

    barrier_signal(me, last)

    @groups
    def _(g):
        for l in LV:
            for c in loads(l, g):
                c.start()
    barrier_wait(me, last)

    @groups
    def _(g):
        send(4, g)
    widen(dw_ref, DW)
    for l in LV:
        zero_edges(S[l], COLS[l])
        if l < END:
            V[l][:, COLS[l]:COLS[l] + TILE, :] = jnp.full((2, TILE, H), NEG, f32)

    @pl.when(me == last)
    def _():
        for l in LV:
            UR[l][:, :1] = jnp.full(shape(l, 1), NEG, bf16)
            UR[l][:, 1:] = jnp.zeros(shape(l, 1), bf16)

    @pl.when(me == 0)
    def _():
        for l in LV:
            DR[l][...] = jnp.zeros(shape(l, 1), bf16)

    for l in LOW:
        rows_first(l, Ph[l], Pv[l], 1, F[l])

    def node(l, g):
        W, R = COLS[l], ROWS[l]
        nb = SLOTS[l]

        def borders(b, ib):
            put_s(S[l], ib, 0, W, fuse(l, b, -1, jnp.maximum(DR[l][b, 0], UP[l][b, 0])))
            put_s(S[l], ib, R, W, fuse(l, b, R - 1, jnp.maximum(Dv[l][b, R - 1], UR[l][b, 0])))
            for c, v in enumerate(halves(UR[l][b, 1].astype(f32))):
                S[l][ib, c, R + 1, cols(W), :] = v

            @pl.when(me == 0)
            def _():
                S[l][ib, :, 0, cols(W), :] = jnp.zeros((2, W, H), f32)

        def pools(b):
            n = R // 2

            def row(r):
                return Ov[l][b, r]
            UP[l + 1][b, 0] = hmax(V[l], row(0), W)

            def pooled(r, inner):
                m = jnp.maximum(row(2 * r), row(2 * r + 1))
                if inner:
                    m = jnp.maximum(m, row(2 * r + 2))
                Dv[l + 1][b, r] = hmax(V[l], m, W)
            if l == TOP:
                @loop(n - 1)
                def _(r):
                    pooled(r, True)
            else:
                for r in range(n - 1):
                    pooled(r, True)
            pooled(n - 1, False)
            first(l + 1, b)

        def before(i):
            b0 = g * N + i * nb
            for ib in range(nb):
                borders(b0 + ib, ib)
            if l == TOP:
                @loop((R - 1) // 3)
                def _(r):
                    for y in THREE:
                        put_s(S[l], 0, 3 * r + y + 1, W, fuse(l, b0, 3 * r + y, Dv[l][b0, 3 * r + y]))
            else:
                for ib in range(nb):
                    for r in range(R - 1):
                        put_s(S[l], ib, r + 1, W, fuse(l, b0 + ib, r, Dv[l][b0 + ib, r]))

        def put(i, ib, o, v):
            Ov[l][g * N + i * nb + ib, o] = v

        def after(i):
            for ib in range(nb):
                pools(g * N + i * nb + ib)
        nq = 4 if l == TOP else 1
        lagged(l, l, N // nb, nq, R // nq, S[l], D, wts, before, put, after if l < END else None)

    def out(l, g):
        return pltpu.make_async_copy(Ov[l].at[sl(g)], Oh[l].at[sl(g)], os.at[l - TOP, g])

    for l in LV:
        @groups
        def _(g):
            if l == TOP:
                for c in loads(l, g):
                    c.wait()
            if l < END:
                for c in loads(l + 1, g):
                    c.wait()
            arrive(l, g)
            node(l, g)
            if l < END:
                send(l + 1, g)
            out(l, g).start()

    for cond, cp in ((me > 0, up), (me < last, dn)):
        @pl.when(cond)
        def _(cp=cp):
            @groups
            def _(g):
                for l in LV:
                    cp(l, g).wait_send()

    @groups
    def _(g):
        for l in LV:
            out(l, g).wait()


def call_bottom_up(n_dev, two, three, p4, qs, xs, ts, d4, h4, wts):
    scratch = [vm(shape(l, ROWS[l] + 1)) for l in LV] + [vm(shape(l, ROWS[l] + 2)) for l in TD]
    scratch += [vm(shape(l, ROWS[l])) for l in LV] * 2 + [vm(shape(l, 2)) for l in LV] * 2 + [vm(shape(l, 1)) for l in LV]
    scratch += [vm((SLOTS[l], 2, ROWS[l] + 2, PADC[l] + 2 * TILE, H), f32) for l in LV] + [vm((2, PADC[l] + TILE, H), f32) for l in TD]
    scratch += [flip_buffer(l) for l in LOW]
    scratch += [vm((2, 24 * 16 + TILE, C)), vm((9, TILE, C), f32), DMA((4, G, 5))] + [DMA((4, G))] * 5
    return pl.pallas_call(
        functools.partial(bottom_up, n_dev=n_dev),
        out_shape=[struct(shape(l, ROWS[l])) for l in LV],
        in_specs=[SMEM] * 2 + [ANY] + [VMEM] * 3 + [ANY] * 9 + [VMEM] * 4,
        out_specs=[ANY] * 4,
        scratch_shapes=scratch,
        compiler_params=pltpu.CompilerParams(collective_id=1, has_side_effects=True, vmem_limit_bytes=62 * MIB),
    )(two, three, p4, *qs, *xs, *ts, d4, h4, *wts)


def finish(i4, i5, i6, i7, o4, o5, o6, o7, buf, F5, F6, F7, si, so):
    def cin(g):
        return pltpu.make_async_copy(i4.at[pl.ds(TWO_N * g, TWO_N)], buf.at[pl.ds(TWO_N * g, TWO_N)], si.at[g])

    def cout(g):
        return pltpu.make_async_copy(buf.at[pl.ds(TWO_N * g, TWO_N)], o4.at[pl.ds(TWO_N * g, TWO_N)], so.at[g])

    @loop(CHUNKS)
    def _(g):
        cin(g).start()
    for l, src, dst, F in ((6, i6, o6, F6), (7, i7, o7, F7), (5, i5, o5, F5)):
        W, R, st = COLS[l], ROWS[l], COLS[l] + 1

        @loop(CHUNKS)
        def _(i):
            if l == 5:
                cin(i).wait()
                cout(i).start()
            for d in TWO:
                b = 2 * i + d
                for r in range(R):
                    for c, v in enumerate(halves(src[b, r].astype(f32))):
                        F[d, c, r * st:r * st + W, :] = v
                for w in range(W):
                    dst[b, w] = join([F[d, c, pl.ds(w, R, stride=st), :] for c in TWO]).astype(bf16)

    @loop(CHUNKS)
    def _(g):
        cout(g).wait()


def call_finish(ins):
    return pl.pallas_call(
        finish,
        out_shape=[struct(shape(4, ROWS[4]))] + [struct(flipped(l)) for l in LOW],
        in_specs=[ANY] + [VMEM] * 3,
        out_specs=[ANY] + [VMEM] * 3,
        scratch_shapes=[vm(shape(4, ROWS[4]))] + [flip_buffer(l) for l in LOW] + [DMA((CHUNKS,))] * 2,
        compiler_params=pltpu.CompilerParams(vmem_limit_bytes=62 * MIB),
    )(*ins)


def flip(a):
    return jnp.swapaxes(a, 1, 2)


def solution(mesh):
    n_dev = mesh.shape['sp']

    def body(p3, p4, p5, p6, p7, fuse_two, fuse_three, dw_filter, pw_weight, bn_scale, bn_bias):
        two, three = fuse_two.T, fuse_three
        qs = [flip(a) for a in (p5, p6, p7)]
        wts = (jnp.transpose(dw_filter, (1, 2, 0, 3)), pw_weight, bn_scale, bn_bias)
        t4, t5, t6, h3, *xs = call_top_down(n_dev, two, three, p3, p4, qs, wts)
        out3, d4, h4 = call_fine(two, three, p3, h3, t4, p4, wts)
        outs = call_bottom_up(n_dev, two, three, p4, qs, xs, (t4, t5, t6), d4, h4, wts)
        out4, *rest = call_finish(outs)
        return out3, out4, *[flip(a) for a in rest]

    band_spec = P('dp', 'sp')
    whole = P()
    return jax.shard_map(body, mesh=mesh, in_specs=(band_spec,) * 5 + (whole,) * 6, out_specs=(band_spec,) * 5, check_vma=False)
```

```python
import functools

import jax
import jax.numpy as jnp
from jax import lax
from jax.experimental import pallas as pl
from jax.experimental.pallas import tpu as pltpu
from jax.sharding import PartitionSpec as P

f32, bf16 = jnp.float32, jnp.bfloat16
FUSE_EPS = 1e-4
B, C, H = 16, 256, 128
G, N = 4, 4
LV = (4, 5, 6, 7)
LOW = LV[1:]
TOP, END = 4, 7
TWO, THREE = range(2), range(3)
ROW0, ROW1 = pl.ds(0, 1), pl.ds(1, 1)
ROWS = {3: 32, 4: 16, 5: 8, 6: 4, 7: 2}
COLS = {3: 80, 4: 40, 5: 20, 6: 10, 7: 5}
PADC = {3: 80, 4: 40, 5: 24, 6: 16, 7: 8}
TILE = CHUNKS = 8
TWO_N = B // CHUNKS
MESH = pl.DeviceIdType.MESH
NEG = -jnp.inf
MIB = 2 ** 20


def groups(fn):
    def body(g, _):
        fn(g)
        return g
    lax.fori_loop(0, G, body, G)


def prev(t):
    return jnp.maximum(t - 1, 0)


def loop(n, unroll=1):
    def run(fn):
        def body(i, _):
            fn(i)
            return i
        lax.fori_loop(0, n, body, n, unroll=unroll)
    return run


def swish(h):
    return h + h * jnp.tanh(h)


def halves(v):
    return v[:, :H], v[:, H:]


def join(v):
    return jnp.concatenate(v, axis=1)


def half(c):
    return slice(c * H, c * H + H)


def cols(W, d=0):
    return slice(TILE + d, TILE + d + W)


def coefs(two, three, k):
    w = [two[i, min(k, 4)] for i in TWO] if k < 4 or k == 7 else [three[k - 4, i] for i in THREE]
    w = [jnp.maximum(x, 0.0) for x in w]
    total = jnp.full((1, C), sum(w[1:], w[0]) + FUSE_EPS, f32)
    return [jnp.full((1, C), 0.5 * x, f32) / total for x in w]


def widen(dw_ref, DW):
    for ky in THREE:
        for kx in THREE:
            DW[3 * ky + kx] = dw_ref[ky, kx].astype(f32)


def tap(DW, k, ky, kx, c):
    return DW[3 * ky + kx, k:k + 1, half(c)]


def zero_edges(S, W):
    S[..., :TILE, :] = jnp.zeros(S.shape[:-2] + (TILE, H), f32)
    S[..., TILE + W:, :] = jnp.zeros(S.shape[:-2] + (S.shape[-2] - TILE - W, H), f32)


def expand(U, v, wc):
    for c, h in enumerate(halves(v)):
        for d in TWO:
            U[c, pl.ds(d, wc, stride=2), :] = h
    return join([U[0], U[1]])


def put_s(S, ib, s, W, h):
    v = swish(h).astype(bf16).astype(f32)
    for c, x in enumerate(halves(v)):
        S[ib, c, s, cols(W), :] = x


def conv_row(S, ib, o, W, DW, k):
    out = []
    for c in TWO:
        acc = None
        for ky in THREE:
            for kx in THREE:
                t = S[ib, c, o + ky, cols(W, kx - 1), :] * tap(DW, k, ky, kx, c)
                acc = t if acc is None else acc + t
        out.append(acc)
    return join(out).astype(bf16)


def lagged(level, k, n, nq, step, S, D, wts, before, put, after):
    DW, pw_ref, sc_ref, bi_ref = wts
    W, wp = COLS[level], PADC[level]
    rows = [(ib, y) for ib in range(S.shape[0]) for y in range(step)]
    m = len(rows) * wp

    def point(t):
        i, q = t // nq, t % nq
        r = jnp.dot(D[t % 2, :m], pw_ref[k], preferred_element_type=f32)
        r = (r * sc_ref[k:k + 1] + bi_ref[k:k + 1]).astype(bf16)
        for x, (ib, y) in enumerate(rows):
            put(i, ib, q * step + y, r[x * wp:x * wp + W])

    def chunk(i, q):
        t = i * nq + q
        point(prev(t))
        for x, (ib, y) in enumerate(rows):
            D[t % 2, x * wp:x * wp + W, :] = conv_row(S, ib, q * step + y, W, DW, k)

    @loop(n)
    def _(i):
        before(i)
        if nq == 1:
            chunk(i, 0)
        else:
            @loop(nq)
            def _(q):
                chunk(i, q)
        if after is not None:
            @pl.when(i > 0)
            def _():
                after(i - 1)
    point(n * nq - 1)
    if after is not None:
        after(n - 1)


def hmax(PV, v, W):
    out = []
    for c, x in enumerate(halves(v.astype(f32))):
        PV[c, :W, :] = x
        a, b, d = [PV[c, pl.ds(i, W // 2, stride=2), :] for i in THREE]
        out.append(jnp.maximum(jnp.maximum(a, b), d))
    return join(out).astype(bf16)


def links(me, last, relay):
    lo, hi = last // 2, last // 2 + 1
    pairs = [(me > 0, me - 1), (me < last, me + 1)]
    if relay:
        for a, b in ((lo, last), (last, hi), (hi, 0), (0, lo)):
            pairs += [(me == a, b), (me == b, a)]
    return pairs


def images(fn):
    @loop(B // len(TWO))
    def _(i):
        for d in TWO:
            fn(len(TWO) * i + d, d)


def rows_first(l, src, dst, off, F):
    W, R, st = COLS[l], ROWS[l], COLS[l] + 1

    @images
    def _(b, d):
        for w in range(W):
            for c, v in enumerate(halves(src[b, w].astype(f32))):
                F[d, c, pl.ds(w, R, stride=st), :] = v
        for r in range(R):
            dst[b, off + r] = join([F[d, c, r * st:r * st + W, :] for c in TWO]).astype(bf16)


def barrier_signal(me, last, relay=False):
    sem = pltpu.get_barrier_semaphore()
    for cond, peer in links(me, last, relay):
        @pl.when(cond)
        def _(peer=peer):
            pl.semaphore_signal(sem, inc=1, device_id={'sp': peer}, device_id_type=MESH)


def barrier_wait(me, last, relay=False):
    sem = pltpu.get_barrier_semaphore()
    for d in range(last + 1):
        @pl.when(me == d)
        def _(d=d):
            pl.semaphore_wait(sem, sum(bool(c) for c, _ in links(d, last, relay)))


def remote(src, dst, ss, rs, dev):
    return pltpu.make_async_remote_copy(src_ref=src, dst_ref=dst, send_sem=ss, recv_sem=rs, device_id={'sp': dev}, device_id_type=MESH)


def shape(l, r):
    return (B, r, COLS[l], C)


def flipped(l):
    return (B, COLS[l], ROWS[l], C)


def vm(s, t=bf16):
    return pltpu.VMEM(s, t)


def flip_buffer(l):
    return vm((2, 2, TILE * -(-ROWS[l] * (COLS[l] + 1) // TILE), H), f32)


DMA = pltpu.SemaphoreType.DMA
ANY = pl.BlockSpec(memory_space=pl.ANY)
VMEM = pl.BlockSpec(memory_space=pltpu.VMEM)
SMEM = pl.BlockSpec(memory_space=pltpu.SMEM)


def struct(s):
    return jax.ShapeDtypeStruct(s, bf16)


def splitter(refs):
    it = iter(refs)

    def take(n):
        return [next(it) for _ in range(n)]
    return take


EXT = {4: 2, 5: 2, 6: 2, 7: 1}
TD = (4, 5, 6)
SLOTS = {4: 1, 5: 1, 6: N, 7: N}


def top_down(*refs, n_dev):
    take = splitter(refs)
    two, three, p3, p4 = take(4)
    Q = dict(zip(LOW, take(3)))
    dw_ref, pw_ref, sc_ref, bi_ref = take(4)
    Th = dict(zip(TD, take(3)))
    h3, = take(1)
    X = dict(zip(LV, take(4)))
    E, T = dict(zip(LV, take(4))), dict(zip(TD, take(3)))
    S, U, F = dict(zip(TD, take(3))), dict(zip(TD, take(3))), dict(zip(LOW, take(3)))
    D, Z, RB, DW, ls, os, xs, s_up, r_up, s_dn, r_dn, s3, r3, zs, rr, fs = take(16)
    lo, hi = (n_dev - 1) // 2, n_dev // 2
    me = lax.axis_index('sp')
    last = n_dev - 1
    wts = (DW, pw_ref, sc_ref, bi_ref)
    FINE_FIRST = (7, 6, 5, 4)

    def sl(g):
        return pl.ds(g * N, N)

    def load(g):
        return pltpu.make_async_copy(p4.at[sl(g)], E[4].at[sl(g), pl.ds(EXT[4], ROWS[4])], ls.at[g])

    def src(l, g, r):
        return p4.at[sl(g), pl.ds(r, EXT[l])] if l == TOP else E[l].at[sl(g), pl.ds(EXT[l] + r, EXT[l])]

    def up(l, g):
        e = EXT[l]
        return remote(src(l, g, 0), E[l].at[sl(g), pl.ds(e + ROWS[l], e)], s_up.at[l - TOP, g], r_up.at[l - TOP, g], me - 1)

    def dn(l, g):
        e = EXT[l]
        return remote(src(l, g, ROWS[l] - e), E[l].at[sl(g), pl.ds(0, e)], s_dn.at[l - TOP, g], r_dn.at[l - TOP, g], me + 1)

    up3 = remote(p3.at[:, ROW0], h3.at[:, ROW1], s3.at[0], r3.at[0], me - 1)
    dn3 = remote(p3.at[:, pl.ds(ROWS[3] - 1, 1)], h3.at[:, ROW0], s3.at[1], r3.at[1], me + 1)

    to_relay = {lo: remote(dn3.src_ref, RB, s3.at[1], rr, last), hi: remote(up3.src_ref, RB, s3.at[0], rr, 0)}
    from_relay = {0: remote(RB, h3.at[:, ROW1], fs, r3.at[0], lo), last: remote(RB, h3.at[:, ROW0], fs, r3.at[1], hi)}
    barrier_signal(me, last, True)

    @groups
    def _(g):
        load(g).start()

    barrier_wait(me, last, True)
    for d, cp in to_relay.items():
        @pl.when(me == d)
        def _(cp=cp):
            cp.start()

    for l in FINE_FIRST[:-1]:
        rows_first(l, Q[l], E[l], EXT[l], F[l])
    Z[...] = jnp.zeros(Z.shape, bf16)
    edge = [pltpu.make_async_copy(Z, h3.at[:, pl.ds(i, 1)], zs) for i in TWO]

    @pl.when(me == 0)
    def _():
        edge[0].start()
        for l in LV:
            E[l][:, :EXT[l]] = jnp.zeros(shape(l, EXT[l]), bf16)

    @pl.when(me == last)
    def _():
        edge[1].start()
        for l in LV:
            E[l][:, EXT[l] + ROWS[l]:] = jnp.zeros(shape(l, EXT[l]), bf16)

    for cond, cp, big, other in ((me > 0, up, up3, hi), (me < last, dn, dn3, lo)):
        @pl.when(cond)
        def _(cp=cp, big=big, other=other):
            @groups
            def _(g):
                for l in FINE_FIRST:
                    cp(l, g).start()

            @pl.when(me != other)
            def _():
                big.start()
    widen(dw_ref, DW)
    for l in TD:
        zero_edges(S[l], COLS[l])

    def node(l, g):
        k = 6 - l
        W, wc, R = COLS[l], COLS[l + 1], ROWS[l]
        a1, a2 = coefs(two, three, k)
        coarse = E[7] if l == 6 else T[l + 1]
        nb = SLOTS[l]

        def fill(b, ib, j, u):
            x = expand(U[l].at[u], coarse[b, j].astype(f32) * a2, wc)
            for d in TWO:
                put_s(S[l], ib, 2 * j + d, W, E[l][b, 2 * j + d].astype(f32) * a1 + x)

        def before(i):
            b0 = g * N + i * nb
            if l == TOP:
                @loop((R + 4) // 4)
                def _(j):
                    for u in TWO:
                        fill(b0, 0, 2 * j + u, u)
            else:
                for ib in range(nb):
                    for j in range((R + 4) // 2):
                        fill(b0 + ib, ib, j, (ib + j) % 2)

        def put(i, ib, o, v):
            T[l][g * N + i * nb + ib, o] = v
        nq = 2 if l == TOP else 1
        lagged(l, k, N // nb, nq, (R + 2) // nq, S[l], D, wts, before, put, None)

        for cond, o in ((me == 0, 0), (me == last, R + 1)):
            @pl.when(cond)
            def _(o=o):
                T[l][sl(g), o:o + 1] = jnp.zeros((N, 1, W, C), bf16)

    def out(l, g):
        return pltpu.make_async_copy(T[l].at[sl(g)], Th[l].at[sl(g)], os.at[l - TOP, g])

    def xout(l):
        return pltpu.make_async_copy(E[l].at[:, pl.ds(EXT[l] - 1, 1)], X[l], xs.at[l - 4])

    def arrive(l, g):
        @pl.when(me > 0)
        def _():
            dn(l, g).wait_recv()

        @pl.when(me < last)
        def _():
            up(l, g).wait_recv()

    @groups
    def _(g):
        arrive(7, g)
        for l in (6, 5, 4):
            if l == TOP:
                load(g).wait()
            arrive(l, g)
            node(l, g)
            out(l, g).start()
        for d, cp in from_relay.items():
            @pl.when((me == d) & (g == 0))
            def _(d=d, cp=cp):
                to_relay[hi if d == 0 else lo].wait_recv()
                cp.start()
    for l in LV:
        xout(l).start()
    for d, cp in from_relay.items():
        @pl.when(me == d)
        def _(cp=cp):
            cp.wait_send()

    for cond, cp, sent, got in ((me > 0, up, up3, dn3), (me < last, dn, dn3, up3)):
        @pl.when(cond)
        def _(cp=cp, sent=sent, got=got):
            @groups
            def _(g):
                for l in LV:
                    cp(l, g).wait_send()
            sent.wait_send()
            got.wait_recv()

    for cond, e in ((me == 0, edge[0]), (me == last, edge[1])):
        @pl.when(cond)
        def _(e=e):
            e.wait()
    for l in LV:
        xout(l).wait()

    @groups
    def _(g):
        for l in TD:
            out(l, g).wait()


def call_top_down(n_dev, two, three, p3, p4, qs, wts):
    scratch = [vm(shape(l, ROWS[l] + 2 * EXT[l])) for l in LV] + [vm(shape(l, ROWS[l] + 2)) for l in TD]
    scratch += [vm((SLOTS[l], 2, ROWS[l] + 4, PADC[l] + 2 * TILE, H), f32) for l in TD]
    scratch += [vm((2, 2, COLS[l], H), f32) for l in TD]
    scratch += [flip_buffer(l) for l in LOW]
    scratch += [vm((2, 24 * 16 + TILE, C)), vm(shape(3, 1)), vm(shape(3, 1)), vm((9, TILE, C), f32)]
    scratch += [DMA((G,)), DMA((3, G)), DMA((4,))] + [DMA((4, G))] * 4 + [DMA((2,))] * 2 + [DMA] * 3
    return pl.pallas_call(
        functools.partial(top_down, n_dev=n_dev),
        out_shape=[struct(shape(l, ROWS[l] + 2)) for l in TD] + [struct(shape(3, 2))] + [struct(shape(l, 1)) for l in LV],
        in_specs=[SMEM] * 2 + [ANY] * 2 + [VMEM] * 7,
        out_specs=[ANY] * 8,
        scratch_shapes=scratch,
        compiler_params=pltpu.CompilerParams(collective_id=0, has_side_effects=True, vmem_limit_bytes=60 * MIB),
    )(two, three, p3, p4, *qs, *wts)


R3, W3 = ROWS[3], COLS[3]
RC3, WC3 = ROWS[4], COLS[4]
PB = 4
NB = RC3 // PB
K3 = 3 * C


def fine(two, three, p_ref, ph_ref, t_ref, p4_ref, t4_ref, dw_ref, pw_ref, sc_ref, bi_ref, o_ref, d_ref, h_ref, S0, S1, U, X0, X1, D0, D1, PV, WD, DW):
    R, W, RC, WC = R3, W3, RC3, WC3
    Xb, Db = (X0, X1), (D0, D1)
    a1, a2 = coefs(two, three, 3)
    b = pl.program_id(0)

    @pl.when(b == 0)
    def _():
        widen(dw_ref, DW)
        zero_edges(S0, W)
        zero_edges(S1, W)
        PV[..., W:, :] = jnp.full((PB, 2, TILE, H), NEG, f32)
        eye = lax.broadcasted_iota(jnp.int32, (H, H), 0) == lax.broadcasted_iota(jnp.int32, (H, H), 1)
        for c in TWO:
            for kx in THREE:
                for pi in TWO:
                    for po in TWO:
                        v = jnp.where(eye, tap(DW, 3, 1 + pi - po, kx, c), 0.0)
                        r0 = kx * C + pi * H
                        WD[c, r0:r0 + H, half(po)] = v.astype(bf16)

    def p1(S, tj, rows, u):
        x = expand(U.at[u], t_ref[tj + 1].astype(f32) * a2, WC)
        for v, si in rows:
            put_s(S, 0, si, W, v.astype(f32) * a1 + x)

    def borders(S):
        p1(S, -1, [(ph_ref[0], 0)], 0)
        p1(S, RC, [(ph_ref[1], R + 1)], 1)

    def act(S, k):
        for t in range(PB):
            tj = k * PB + t
            p1(S, tj, [(p_ref[2 * tj + d], 2 * tj + d + 1) for d in TWO], t % 2)

    def gather(S, X, k):
        for c in TWO:
            for p in range(PB):
                for kx in THREE:
                    X[c, p * W:(p + 1) * W, kx * C:kx * C + C] = join(
                        [S[0, c, 2 * (k * PB + p) + 1 + par, cols(W, kx - 1), :] for par in TWO]).astype(bf16)

    def conv(S, X, D, k):
        for c in TWO:
            r = jnp.dot(X[c, :PB * W], WD[c], preferred_element_type=f32)
            for p in range(PB):
                for par in TWO:
                    si = 2 * (k * PB + p) + 3 * par
                    q = r[p * W:(p + 1) * W, half(par)]
                    for kx in THREE:
                        q = q + S[0, c, si, cols(W, kx - 1), :] * tap(DW, 3, 2 * par, kx, c)
                    y = 2 * p + par
                    D[y * W:(y + 1) * W, half(c)] = q.astype(bf16)

    def point(D, k):
        o = jnp.dot(D[:2 * PB * W], pw_ref[3], preferred_element_type=f32)
        o = (o * sc_ref[3:4] + bi_ref[3:4]).astype(bf16)
        for y in range(2 * PB):
            o_ref[2 * PB * k + y] = o[y * W:(y + 1) * W]

    def step(Sn, Sp):
        if Sn is not None:
            borders(Sn)
        for k in range(NB):
            u = k % 2
            conv(Sp, Xb[u], Db[u], k)
            if k:
                point(Db[1 - u], k - 1)
            if k < NB - 1:
                gather(Sp, Xb[1 - u], k + 1)
            elif Sn is not None:
                gather(Sn, Xb[1 - u], 0)
            if Sn is not None:
                act(Sn, k)
        point(Db[1], NB - 1)

    @pl.when(b == 0)
    def _():
        borders(S0)

        @loop(NB)
        def _(k):
            act(S0, k)
        gather(S0, X0, 0)

    inner = (b > 0) & (b < B)

    @pl.when(inner & (b % 2 == 0))
    def _():
        step(S0, S1)

    @pl.when(inner & (b % 2 == 1))
    def _():
        step(S1, S0)

    @pl.when(b == B)
    def _():
        step(None, S1)

    @pl.when(b > 0)
    def _():
        h_ref[0] = hmax(PV.at[0], o_ref[0], W)

        @loop(RC // PB)
        def _(q):
            for y in range(PB):
                r = q * PB + y
                rn = jnp.minimum(2 * r + 2, R - 1)
                d_ref[r] = hmax(PV.at[y], jnp.maximum(jnp.maximum(o_ref[2 * r], o_ref[2 * r + 1]), o_ref[rn]), W)
        a = coefs(two, three, TOP)
        maps = (p4_ref[0], t4_ref[0], d_ref[0])
        h_ref[1] = swish(sum(x.astype(f32) * y for x, y in zip(maps, a))).astype(bf16)


def call_fine(two, three, p, ph, t, p4, wts):
    def block(s, late=False, row=0):
        return pl.BlockSpec((None,) + s[1:], lambda b: (prev(b) if late else jnp.minimum(b, B - 1), row, 0, 0))
    full = [pl.BlockSpec(a.shape, lambda b, n=a.ndim: (0,) * n) for a in wts]
    outs = [shape(3, R3), shape(4, RC3), shape(4, 2)]
    S = vm((1, 2, R3 + 2, W3 + 2 * TILE, H), f32)
    X = vm((2, PB * W3 + TILE, K3))
    D = vm((2 * PB * W3 + TILE, C))
    return pl.pallas_call(
        fine, grid=(B + 1,),
        out_shape=[struct(s) for s in outs],
        in_specs=[SMEM] * 2 + [block(a.shape) for a in (p, ph, t)] + [block(shape(4, 1), True, r) for r in TWO] + full,
        out_specs=[block(s, True) for s in outs],
        scratch_shapes=[S, S, vm((2, 2, W3, H), f32), X, X, D, D, vm((PB, 2, W3 + TILE, H), f32), vm((2, K3, C)), vm((9, TILE, C), f32)],
        compiler_params=pltpu.CompilerParams(vmem_limit_bytes=60 * MIB),
    )(two, three, p, ph, t, p4, t, *wts)


def bottom_up(*refs, n_dev):
    take = splitter(refs)
    two, three, p4 = take(3)
    Ph = {4: p4, **dict(zip(LOW, take(3)))}
    Xh, Th = dict(zip(LV, take(4))), dict(zip(TD, take(3)))
    d4, h4, dw_ref, pw_ref, sc_ref, bi_ref = take(6)
    Oh = dict(zip(LV, take(4)))
    Pv, Tv, Dv, Ov = dict(zip(LV, take(4))), dict(zip(TD, take(3))), dict(zip(LV, take(4))), dict(zip(LV, take(4)))
    UP, UR, DR, S = [dict(zip(LV, take(4))) for _ in range(4)]
    V = dict(zip(TD, take(3)))
    F = dict(zip(LOW, take(3)))
    D, DW, ls, os, s_up, r_up, s_dn, r_dn = take(8)
    me = lax.axis_index('sp')
    last = n_dev - 1
    wts = (DW, pw_ref, sc_ref, bi_ref)

    def sl(g):
        return pl.ds(g * N, N)

    def loads(l, g):
        q = sl(g)
        pairs = [(Xh[l].at[q], Pv[l].at[q, ROW0])]
        if l == TOP:
            pairs += [(p4.at[q], Pv[4].at[q, pl.ds(1, ROWS[4])]), (d4.at[q], Dv[4].at[q]), (h4.at[q], UP[4].at[q])]
        if l < END:
            pairs += [(Th[l].at[q], Tv[l].at[q])]
        return [pltpu.make_async_copy(a, b, ls.at[l - TOP, g, i]) for i, (a, b) in enumerate(pairs)]

    def up(l, g):
        return remote((h4 if l == TOP else UP[l]).at[sl(g)], UR[l].at[sl(g)], s_up.at[l - TOP, g], r_up.at[l - TOP, g], me - 1)

    def dn(l, g):
        return remote((d4 if l == TOP else Dv[l]).at[sl(g), pl.ds(ROWS[l] - 1, 1)], DR[l].at[sl(g)], s_dn.at[l - TOP, g], r_dn.at[l - TOP, g], me + 1)

    def send(l, g):
        @pl.when(me > 0)
        def _():
            up(l, g).start()

        @pl.when(me < last)
        def _():
            dn(l, g).start()

    def arrive(l, g):
        @pl.when(me < last)
        def _():
            up(l, g).wait_recv()

        @pl.when(me > 0)
        def _():
            dn(l, g).wait_recv()

    CF = {l: coefs(two, three, l) for l in LV}

    def fuse(l, b, r, d):
        a = CF[l]
        h = Pv[l][b, r + 1].astype(f32) * a[0] + d.astype(f32) * a[-1]
        if l < END:
            h = h + Tv[l][b, r + 1].astype(f32) * a[1]
        return h

    def first(l, b):
        UP[l][b, 1] = swish(fuse(l, b, 0, Dv[l][b, 0])).astype(bf16)

    barrier_signal(me, last)

    @groups
    def _(g):
        for l in LV:
            for c in loads(l, g):
                c.start()
    barrier_wait(me, last)

    @groups
    def _(g):
        send(4, g)
    widen(dw_ref, DW)
    for l in LV:
        zero_edges(S[l], COLS[l])
        if l < END:
            V[l][:, COLS[l]:COLS[l] + TILE, :] = jnp.full((2, TILE, H), NEG, f32)

    @pl.when(me == last)
    def _():
        for l in LV:
            UR[l][:, :1] = jnp.full(shape(l, 1), NEG, bf16)
            UR[l][:, 1:] = jnp.zeros(shape(l, 1), bf16)

    @pl.when(me == 0)
    def _():
        for l in LV:
            DR[l][...] = jnp.zeros(shape(l, 1), bf16)

    for l in LOW:
        rows_first(l, Ph[l], Pv[l], 1, F[l])

    def node(l, g):
        W, R = COLS[l], ROWS[l]
        nb = SLOTS[l]

        def borders(b, ib):
            put_s(S[l], ib, 0, W, fuse(l, b, -1, jnp.maximum(DR[l][b, 0], UP[l][b, 0])))
            put_s(S[l], ib, R, W, fuse(l, b, R - 1, jnp.maximum(Dv[l][b, R - 1], UR[l][b, 0])))
            for c, v in enumerate(halves(UR[l][b, 1].astype(f32))):
                S[l][ib, c, R + 1, cols(W), :] = v

            @pl.when(me == 0)
            def _():
                S[l][ib, :, 0, cols(W), :] = jnp.zeros((2, W, H), f32)

        def pools(b):
            n = R // 2

            def row(r):
                return Ov[l][b, r]
            UP[l + 1][b, 0] = hmax(V[l], row(0), W)

            def pooled(r, inner):
                m = jnp.maximum(row(2 * r), row(2 * r + 1))
                if inner:
                    m = jnp.maximum(m, row(2 * r + 2))
                Dv[l + 1][b, r] = hmax(V[l], m, W)
            if l == TOP:
                @loop(n - 1)
                def _(r):
                    pooled(r, True)
            else:
                for r in range(n - 1):
                    pooled(r, True)
            pooled(n - 1, False)
            first(l + 1, b)

        def before(i):
            b0 = g * N + i * nb
            for ib in range(nb):
                borders(b0 + ib, ib)
            if l == TOP:
                @loop(len(THREE))
                def _(q):
                    for y in range(5):
                        r = 5 * q + y
                        put_s(S[l], 0, r + 1, W, fuse(l, b0, r, Dv[l][b0, r]))
            else:
                for ib in range(nb):
                    for r in range(R - 1):
                        put_s(S[l], ib, r + 1, W, fuse(l, b0 + ib, r, Dv[l][b0 + ib, r]))

        def put(i, ib, o, v):
            Ov[l][g * N + i * nb + ib, o] = v

        def after(i):
            for ib in range(nb):
                pools(g * N + i * nb + ib)
        nq = 2 if l == TOP else 1
        lagged(l, l, N // nb, nq, R // nq, S[l], D, wts, before, put, after if l < END else None)

    def out(l, g):
        return pltpu.make_async_copy(Ov[l].at[sl(g)], Oh[l].at[sl(g)], os.at[l - TOP, g])

    for l in LV:
        @groups
        def _(g):
            if l == TOP:
                for c in loads(l, g):
                    c.wait()
            if l < END:
                for c in loads(l + 1, g):
                    c.wait()
            arrive(l, g)
            node(l, g)
            if l < END:
                send(l + 1, g)
            out(l, g).start()

    for cond, cp in ((me > 0, up), (me < last, dn)):
        @pl.when(cond)
        def _(cp=cp):
            @groups
            def _(g):
                for l in LV:
                    cp(l, g).wait_send()

    @groups
    def _(g):
        for l in LV:
            out(l, g).wait()


def call_bottom_up(n_dev, two, three, p4, qs, xs, ts, d4, h4, wts):
    scratch = [vm(shape(l, ROWS[l] + 1)) for l in LV] + [vm(shape(l, ROWS[l] + 2)) for l in TD]
    scratch += [vm(shape(l, ROWS[l])) for l in LV] * 2 + [vm(shape(l, 2)) for l in LV] * 2 + [vm(shape(l, 1)) for l in LV]
    scratch += [vm((SLOTS[l], 2, ROWS[l] + 2, PADC[l] + 2 * TILE, H), f32) for l in LV] + [vm((2, PADC[l] + TILE, H), f32) for l in TD]
    scratch += [flip_buffer(l) for l in LOW]
    scratch += [vm((2, 24 * 16 + TILE, C)), vm((9, TILE, C), f32), DMA((4, G, 5))] + [DMA((4, G))] * 5
    return pl.pallas_call(
        functools.partial(bottom_up, n_dev=n_dev),
        out_shape=[struct(shape(l, ROWS[l])) for l in LV],
        in_specs=[SMEM] * 2 + [ANY] + [VMEM] * 3 + [ANY] * 9 + [VMEM] * 4,
        out_specs=[ANY] * 4,
        scratch_shapes=scratch,
        compiler_params=pltpu.CompilerParams(collective_id=1, has_side_effects=True, vmem_limit_bytes=62 * MIB),
    )(two, three, p4, *qs, *xs, *ts, d4, h4, *wts)


def finish(*refs):
    take = splitter(refs)
    src, dst, got, put, F = [dict(zip(LV, take(4))) for _ in range(4)] + [dict(zip(LOW, take(3)))]
    si, so, ti, to = take(4)
    top = got[TOP]

    def piece(g):
        return pl.ds(TWO_N * g, TWO_N)

    def cin(g):
        return pltpu.make_async_copy(src[TOP].at[piece(g)], top.at[piece(g)], si.at[g])

    def cout(g):
        return pltpu.make_async_copy(top.at[piece(g)], dst[TOP].at[piece(g)], so.at[g])

    def small_in(l):
        return pltpu.make_async_copy(src[l], got[l], ti.at[l - TOP])

    def small_out(l):
        return pltpu.make_async_copy(put[l], dst[l], to.at[l - TOP])

    for l in LOW[::-1]:
        small_in(l).start()

    @loop(CHUNKS)
    def _(g):
        cin(g).start()
    for l in LOW[::-1]:
        W, R, st = COLS[l], ROWS[l], COLS[l] + 1
        small_in(l).wait()

        @loop(CHUNKS)
        def _(i):
            if l == LOW[0]:
                cin(i).wait()
                cout(i).start()
            for d in TWO:
                b = 2 * i + d
                for r in range(R):
                    for c, v in enumerate(halves(got[l][b, r].astype(f32))):
                        F[l][d, c, r * st:r * st + W, :] = v
                for w in range(W):
                    put[l][b, w] = join([F[l][d, c, pl.ds(w, R, stride=st), :] for c in TWO]).astype(bf16)
        small_out(l).start()
    for l in LOW:
        small_out(l).wait()

    @loop(CHUNKS)
    def _(g):
        cout(g).wait()


def call_finish(ins):
    outs = [shape(4, ROWS[4])] + [flipped(l) for l in LOW]
    return pl.pallas_call(
        finish,
        out_shape=[struct(x) for x in outs],
        in_specs=[ANY] * 4,
        out_specs=[ANY] * 4,
        scratch_shapes=[vm(a.shape) for a in ins] + [vm((TILE, H))] + [vm(x) for x in outs[1:]] + [flip_buffer(l) for l in LOW]
        + [DMA((CHUNKS,))] * 2 + [DMA((4,))] * 2,
        compiler_params=pltpu.CompilerParams(vmem_limit_bytes=62 * MIB),
    )(*ins)


def flip(a):
    return jnp.swapaxes(a, 1, 2)


def solution(mesh):
    n_dev = mesh.shape['sp']

    def body(p3, p4, p5, p6, p7, fuse_two, fuse_three, dw_filter, pw_weight, bn_scale, bn_bias):
        two, three = fuse_two.T, fuse_three
        qs = [flip(a) for a in (p5, p6, p7)]
        wts = (jnp.transpose(dw_filter, (1, 2, 0, 3)), pw_weight, bn_scale, bn_bias)
        t4, t5, t6, h3, *xs = call_top_down(n_dev, two, three, p3, p4, qs, wts)
        out3, d4, h4 = call_fine(two, three, p3, h3, t4, p4, wts)
        outs = call_bottom_up(n_dev, two, three, p4, qs, xs, (t4, t5, t6), d4, h4, wts)
        out4, *rest = call_finish(outs)
        return out3, out4, *[flip(a) for a in rest]

    band_spec = P('dp', 'sp')
    whole = P()
    return jax.shard_map(body, mesh=mesh, in_specs=(band_spec,) * 5 + (whole,) * 6, out_specs=(band_spec,) * 5, check_vma=False)
```

```python
import functools

import jax
import jax.numpy as jnp
from jax import lax
from jax.experimental import pallas as pl
from jax.experimental.pallas import tpu as pltpu
from jax.sharding import PartitionSpec as P

f32, bf16 = jnp.float32, jnp.bfloat16
FUSE_EPS = 1e-4
B, C, H = 16, 256, 128
G, N = 4, 4
LV = (4, 5, 6, 7)
LOW = LV[1:]
TOP, END = 4, 7
TWO, THREE = range(2), range(3)
ROW0, ROW1 = pl.ds(0, 1), pl.ds(1, 1)
ROWS = {3: 32, 4: 16, 5: 8, 6: 4, 7: 2}
COLS = {3: 80, 4: 40, 5: 20, 6: 10, 7: 5}
PADC = {3: 80, 4: 40, 5: 24, 6: 16, 7: 8}
TILE = CHUNKS = 8
TWO_N = B // CHUNKS
MESH = pl.DeviceIdType.MESH
NEG = -jnp.inf
MIB = 2 ** 20


def groups(fn):
    def body(g, _):
        fn(g)
        return g
    lax.fori_loop(0, G, body, G)


def prev(t):
    return jnp.maximum(t - 1, 0)


def loop(n, unroll=1):
    def run(fn):
        def body(i, _):
            fn(i)
            return i
        lax.fori_loop(0, n, body, n, unroll=unroll)
    return run


def swish(h):
    return h + h * jnp.tanh(h)


def halves(v):
    return v[:, :H], v[:, H:]


def join(v):
    return jnp.concatenate(v, axis=1)


def half(c):
    return slice(c * H, c * H + H)


def cols(W, d=0):
    return slice(TILE + d, TILE + d + W)


def coefs(two, three, k):
    w = [two[i, min(k, 4)] for i in TWO] if k < 4 or k == 7 else [three[k - 4, i] for i in THREE]
    w = [jnp.maximum(x, 0.0) for x in w]
    total = jnp.full((1, C), sum(w[1:], w[0]) + FUSE_EPS, f32)
    return [jnp.full((1, C), 0.5 * x, f32) / total for x in w]


def widen(dw_ref, DW):
    for ky in THREE:
        for kx in THREE:
            DW[3 * ky + kx] = dw_ref[ky, kx].astype(f32)


def tap(DW, k, ky, kx, c):
    return DW[3 * ky + kx, k:k + 1, half(c)]


def zero_edges(S, W):
    S[..., :TILE, :] = jnp.zeros(S.shape[:-2] + (TILE, H), f32)
    S[..., TILE + W:, :] = jnp.zeros(S.shape[:-2] + (S.shape[-2] - TILE - W, H), f32)


def expand(U, v, wc):
    for c, h in enumerate(halves(v)):
        for d in TWO:
            U[c, pl.ds(d, wc, stride=2), :] = h
    return join([U[0], U[1]])


def put_s(S, ib, s, W, h):
    v = swish(h).astype(bf16).astype(f32)
    for c, x in enumerate(halves(v)):
        S[ib, c, s, cols(W), :] = x


def conv_row(S, ib, o, W, DW, k):
    out = []
    for c in TWO:
        acc = None
        for ky in THREE:
            for kx in THREE:
                t = S[ib, c, o + ky, cols(W, kx - 1), :] * tap(DW, k, ky, kx, c)
                acc = t if acc is None else acc + t
        out.append(acc)
    return join(out).astype(bf16)


def lagged(level, k, n, nq, step, S, D, wts, before, put, after):
    DW, pw_ref, sc_ref, bi_ref = wts
    W, wp = COLS[level], PADC[level]
    rows = [(ib, y) for ib in range(S.shape[0]) for y in range(step)]
    m = len(rows) * wp

    def point(t):
        i, q = t // nq, t % nq
        r = jnp.dot(D[t % 2, :m], pw_ref[k], preferred_element_type=f32)
        r = (r * sc_ref[k:k + 1] + bi_ref[k:k + 1]).astype(bf16)
        for x, (ib, y) in enumerate(rows):
            put(i, ib, q * step + y, r[x * wp:x * wp + W])

    def chunk(i, q):
        t = i * nq + q
        point(prev(t))
        for x, (ib, y) in enumerate(rows):
            D[t % 2, x * wp:x * wp + W, :] = conv_row(S, ib, q * step + y, W, DW, k)

    @loop(n)
    def _(i):
        before(i)
        if nq == 1:
            chunk(i, 0)
        else:
            @loop(nq)
            def _(q):
                chunk(i, q)
        if after is not None:
            @pl.when(i > 0)
            def _():
                after(i - 1)
    point(n * nq - 1)
    if after is not None:
        after(n - 1)


def hmax(PV, v, W):
    out = []
    for c, x in enumerate(halves(v.astype(f32))):
        PV[c, :W, :] = x
        a, b, d = [PV[c, pl.ds(i, W // 2, stride=2), :] for i in THREE]
        out.append(jnp.maximum(jnp.maximum(a, b), d))
    return join(out).astype(bf16)


def links(me, last, relay):
    lo, hi = last // 2, last // 2 + 1
    pairs = [(me > 0, me - 1), (me < last, me + 1)]
    if relay:
        for a, b in ((lo, last), (last, hi), (hi, 0), (0, lo)):
            pairs += [(me == a, b), (me == b, a)]
    return pairs


def images(fn):
    @loop(B // len(TWO))
    def _(i):
        for d in TWO:
            fn(len(TWO) * i + d, d)


def rows_first(l, src, dst, off, F):
    W, R, st = COLS[l], ROWS[l], COLS[l] + 1

    @images
    def _(b, d):
        for w in range(W):
            for c, v in enumerate(halves(src[b, w].astype(f32))):
                F[d, c, pl.ds(w, R, stride=st), :] = v
        for r in range(R):
            dst[b, off + r] = join([F[d, c, r * st:r * st + W, :] for c in TWO]).astype(bf16)


def barrier_signal(me, last, relay=False):
    sem = pltpu.get_barrier_semaphore()
    for cond, peer in links(me, last, relay):
        @pl.when(cond)
        def _(peer=peer):
            pl.semaphore_signal(sem, inc=1, device_id={'sp': peer}, device_id_type=MESH)


def barrier_wait(me, last, relay=False):
    sem = pltpu.get_barrier_semaphore()
    for d in range(last + 1):
        @pl.when(me == d)
        def _(d=d):
            pl.semaphore_wait(sem, sum(bool(c) for c, _ in links(d, last, relay)))


def remote(src, dst, ss, rs, dev):
    return pltpu.make_async_remote_copy(src_ref=src, dst_ref=dst, send_sem=ss, recv_sem=rs, device_id={'sp': dev}, device_id_type=MESH)


def shape(l, r):
    return (B, r, COLS[l], C)


def flipped(l):
    return (B, COLS[l], ROWS[l], C)


def vm(s, t=bf16):
    return pltpu.VMEM(s, t)


def product_rows():
    return vm((2, 24 * 16 + TILE, C))


def flip_buffer(l):
    return vm((2, 2, TILE * -(-ROWS[l] * (COLS[l] + 1) // TILE), H), f32)


DMA = pltpu.SemaphoreType.DMA
ANY = pl.BlockSpec(memory_space=pl.ANY)
VMEM = pl.BlockSpec(memory_space=pltpu.VMEM)
SMEM = pl.BlockSpec(memory_space=pltpu.SMEM)


def struct(s):
    return jax.ShapeDtypeStruct(s, bf16)


def splitter(refs):
    it = iter(refs)

    def take(n):
        return [next(it) for _ in range(n)]
    return take


EXT = dict(zip(LV, (2, 2, 2, 1)))
TD = (4, 5, 6)
SLOTS = dict(zip(LV, (1, 1, N, N)))


def top_down(*refs, n_dev):
    take = splitter(refs)
    two, three, p3, p4 = take(4)
    Q = dict(zip(LOW, take(3)))
    dw_ref, pw_ref, sc_ref, bi_ref = take(4)
    Th = dict(zip(TD, take(3)))
    h3, = take(1)
    X = dict(zip(LV, take(4)))
    E, T = dict(zip(LV, take(4))), dict(zip(TD, take(3)))
    S, U, F = dict(zip(TD, take(3))), dict(zip(TD, take(3))), dict(zip(LOW, take(3)))
    D, Z, RB, DW, ls, os, xs, s_up, r_up, s_dn, r_dn, s3, r3, zs, rr, fs = take(16)
    lo, hi = (n_dev - 1) // 2, n_dev // 2
    me = lax.axis_index('sp')
    last = n_dev - 1
    wts = (DW, pw_ref, sc_ref, bi_ref)
    FINE_FIRST = (7, 6, 5, 4)

    def sl(g):
        return pl.ds(g * N, N)

    def load(g):
        return pltpu.make_async_copy(p4.at[sl(g)], E[4].at[sl(g), pl.ds(EXT[4], ROWS[4])], ls.at[g])

    def src(l, g, r):
        return p4.at[sl(g), pl.ds(r, EXT[l])] if l == TOP else E[l].at[sl(g), pl.ds(EXT[l] + r, EXT[l])]

    def up(l, g):
        e = EXT[l]
        return remote(src(l, g, 0), E[l].at[sl(g), pl.ds(e + ROWS[l], e)], s_up.at[l - TOP, g], r_up.at[l - TOP, g], me - 1)

    def dn(l, g):
        e = EXT[l]
        return remote(src(l, g, ROWS[l] - e), E[l].at[sl(g), pl.ds(0, e)], s_dn.at[l - TOP, g], r_dn.at[l - TOP, g], me + 1)

    up3 = remote(p3.at[:, ROW0], h3.at[:, ROW1], s3.at[0], r3.at[0], me - 1)
    dn3 = remote(p3.at[:, pl.ds(ROWS[3] - 1, 1)], h3.at[:, ROW0], s3.at[1], r3.at[1], me + 1)

    to_relay = {lo: remote(dn3.src_ref, RB, s3.at[1], rr, last), hi: remote(up3.src_ref, RB, s3.at[0], rr, 0)}
    from_relay = {0: remote(RB, h3.at[:, ROW1], fs, r3.at[0], lo), last: remote(RB, h3.at[:, ROW0], fs, r3.at[1], hi)}
    barrier_signal(me, last, True)

    @groups
    def _(g):
        load(g).start()

    barrier_wait(me, last, True)
    for d, cp in to_relay.items():
        @pl.when(me == d)
        def _(cp=cp):
            cp.start()
    for cond, cp in ((me > 0, up), (me < last, dn)):
        @pl.when(cond)
        def _(cp=cp):
            cp(TOP, 0).start()

    for l in FINE_FIRST[:-1]:
        rows_first(l, Q[l], E[l], EXT[l], F[l])
    Z[...] = jnp.zeros(Z.shape, bf16)
    edge = [pltpu.make_async_copy(Z, h3.at[:, pl.ds(i, 1)], zs) for i in TWO]

    @pl.when(me == 0)
    def _():
        edge[0].start()
        for l in LV:
            E[l][:, :EXT[l]] = jnp.zeros(shape(l, EXT[l]), bf16)

    @pl.when(me == last)
    def _():
        edge[1].start()
        for l in LV:
            E[l][:, EXT[l] + ROWS[l]:] = jnp.zeros(shape(l, EXT[l]), bf16)

    for cond, cp, big, other in ((me > 0, up, up3, hi), (me < last, dn, dn3, lo)):
        @pl.when(cond)
        def _(cp=cp, big=big, other=other):
            @groups
            def _(g):
                for l in FINE_FIRST[:-1]:
                    cp(l, g).start()

                @pl.when(g > 0)
                def _():
                    cp(TOP, g).start()

            @pl.when(me != other)
            def _():
                big.start()
    widen(dw_ref, DW)
    for l in TD:
        zero_edges(S[l], COLS[l])

    def node(l, g):
        k = 6 - l
        W, wc, R = COLS[l], COLS[l + 1], ROWS[l]
        a1, a2 = coefs(two, three, k)
        coarse = E[7] if l == 6 else T[l + 1]
        nb = SLOTS[l]

        def fill(b, ib, j, u):
            x = expand(U[l].at[u], coarse[b, j].astype(f32) * a2, wc)
            for d in TWO:
                put_s(S[l], ib, 2 * j + d, W, E[l][b, 2 * j + d].astype(f32) * a1 + x)

        def before(i):
            b0 = g * N + i * nb
            if l == TOP:
                @loop((R + 4) // 4)
                def _(j):
                    for u in TWO:
                        fill(b0, 0, 2 * j + u, u)
            else:
                for ib in range(nb):
                    for j in range((R + 4) // 2):
                        fill(b0 + ib, ib, j, (ib + j) % 2)

        def put(i, ib, o, v):
            T[l][g * N + i * nb + ib, o] = v
        nq = 2 if l == TOP else 1
        lagged(l, k, N // nb, nq, (R + 2) // nq, S[l], D, wts, before, put, None)

        for cond, o in ((me == 0, 0), (me == last, R + 1)):
            @pl.when(cond)
            def _(o=o):
                T[l][sl(g), o:o + 1] = jnp.zeros((N, 1, W, C), bf16)

    def out(l, g):
        return pltpu.make_async_copy(T[l].at[sl(g)], Th[l].at[sl(g)], os.at[l - TOP, g])

    def xout(l):
        return pltpu.make_async_copy(E[l].at[:, pl.ds(EXT[l] - 1, 1)], X[l], xs.at[l - 4])

    def arrive(l, g):
        @pl.when(me > 0)
        def _():
            dn(l, g).wait_recv()

        @pl.when(me < last)
        def _():
            up(l, g).wait_recv()

    @groups
    def _(g):
        arrive(7, g)
        for l in (6, 5, 4):
            if l == TOP:
                load(g).wait()
            arrive(l, g)
            node(l, g)
            out(l, g).start()
        for d, cp in from_relay.items():
            @pl.when((me == d) & (g == 0))
            def _(d=d, cp=cp):
                to_relay[hi if d == 0 else lo].wait_recv()
                cp.start()
    for l in LV:
        xout(l).start()
    for d, cp in from_relay.items():
        @pl.when(me == d)
        def _(cp=cp):
            cp.wait_send()

    for cond, cp, sent, got in ((me > 0, up, up3, dn3), (me < last, dn, dn3, up3)):
        @pl.when(cond)
        def _(cp=cp, sent=sent, got=got):
            @groups
            def _(g):
                for l in LV:
                    cp(l, g).wait_send()
            sent.wait_send()
            got.wait_recv()

    for cond, e in ((me == 0, edge[0]), (me == last, edge[1])):
        @pl.when(cond)
        def _(e=e):
            e.wait()
    for l in LV:
        xout(l).wait()

    @groups
    def _(g):
        for l in TD:
            out(l, g).wait()


def call_top_down(n_dev, two, three, p3, p4, qs, wts):
    scratch = [vm(shape(l, ROWS[l] + 2 * EXT[l])) for l in LV] + [vm(shape(l, ROWS[l] + 2)) for l in TD]
    scratch += [vm((SLOTS[l], 2, ROWS[l] + 4, PADC[l] + 2 * TILE, H), f32) for l in TD]
    scratch += [vm((2, 2, COLS[l], H), f32) for l in TD]
    scratch += [flip_buffer(l) for l in LOW]
    scratch += [product_rows(), vm(shape(3, 1)), vm(shape(3, 1)), vm((9, TILE, C), f32)]
    scratch += [DMA((G,)), DMA((3, G)), DMA((4,))] + [DMA((4, G))] * 4 + [DMA((2,))] * 2 + [DMA] * 3
    return pl.pallas_call(
        functools.partial(top_down, n_dev=n_dev),
        out_shape=[struct(shape(l, ROWS[l] + 2)) for l in TD] + [struct(shape(3, 2))] + [struct(shape(l, 1)) for l in LV],
        in_specs=[SMEM] * 2 + [ANY] * 2 + [VMEM] * 7,
        out_specs=[ANY] * 8,
        scratch_shapes=scratch,
        compiler_params=pltpu.CompilerParams(collective_id=0, has_side_effects=True, vmem_limit_bytes=60 * MIB),
    )(two, three, p3, p4, *qs, *wts)


R3, W3 = ROWS[3], COLS[3]
RC3, WC3 = ROWS[4], COLS[4]
PB = 4
NB = RC3 // PB
K3 = 3 * C


def fine(two, three, p_ref, ph_ref, t_ref, p4_ref, t4_ref, dw_ref, pw_ref, sc_ref, bi_ref, o_ref, d_ref, h_ref, S0, S1, U, X0, X1, D0, D1, PV, WD, DW):
    R, W, RC, WC = R3, W3, RC3, WC3
    Xb, Db = (X0, X1), (D0, D1)
    a1, a2 = coefs(two, three, 3)
    b = pl.program_id(0)

    @pl.when(b == 0)
    def _():
        widen(dw_ref, DW)
        zero_edges(S0, W)
        zero_edges(S1, W)
        PV[..., W:, :] = jnp.full((PB, 2, TILE, H), NEG, f32)
        eye = lax.broadcasted_iota(jnp.int32, (H, H), 0) == lax.broadcasted_iota(jnp.int32, (H, H), 1)
        for c in TWO:
            for kx in THREE:
                for pi in TWO:
                    for po in TWO:
                        v = jnp.where(eye, tap(DW, 3, 1 + pi - po, kx, c), 0.0)
                        r0 = kx * C + pi * H
                        WD[c, r0:r0 + H, half(po)] = v.astype(bf16)

    def p1(S, tj, rows, u):
        x = expand(U.at[u], t_ref[tj + 1].astype(f32) * a2, WC)
        for v, si in rows:
            put_s(S, 0, si, W, v.astype(f32) * a1 + x)

    def borders(S):
        p1(S, -1, [(ph_ref[0], 0)], 0)
        p1(S, RC, [(ph_ref[1], R + 1)], 1)

    def act(S, k):
        for t in range(PB):
            tj = k * PB + t
            p1(S, tj, [(p_ref[2 * tj + d], 2 * tj + d + 1) for d in TWO], t % 2)

    def gather(S, X, k):
        for c in TWO:
            for p in range(PB):
                for kx in THREE:
                    X[c, p * W:(p + 1) * W, kx * C:kx * C + C] = join(
                        [S[0, c, 2 * (k * PB + p) + 1 + par, cols(W, kx - 1), :] for par in TWO]).astype(bf16)

    def conv(S, X, D, k):
        for c in TWO:
            r = jnp.dot(X[c, :PB * W], WD[c], preferred_element_type=f32)
            for p in range(PB):
                for par in TWO:
                    si = 2 * (k * PB + p) + 3 * par
                    q = r[p * W:(p + 1) * W, half(par)]
                    for kx in THREE:
                        q = q + S[0, c, si, cols(W, kx - 1), :] * tap(DW, 3, 2 * par, kx, c)
                    y = 2 * p + par
                    D[y * W:(y + 1) * W, half(c)] = q.astype(bf16)

    def point(D, k):
        o = jnp.dot(D[:2 * PB * W], pw_ref[3], preferred_element_type=f32)
        o = (o * sc_ref[3:4] + bi_ref[3:4]).astype(bf16)
        for y in range(2 * PB):
            o_ref[2 * PB * k + y] = o[y * W:(y + 1) * W]

    def pool(k):
        for y in range(PB):
            r = PB * k - 1 + y
            if r >= 0:
                m = jnp.maximum(jnp.maximum(o_ref[2 * r], o_ref[2 * r + 1]), o_ref[2 * r + 2])
                d_ref[r] = hmax(PV.at[y], m, W)

    def step(Sn, Sp):
        if Sn is not None:
            borders(Sn)
        for k in range(NB):
            u = k % 2
            conv(Sp, Xb[u], Db[u], k)
            if k:
                point(Db[1 - u], k - 1)
                pool(k - 1)
            if k < NB - 1:
                gather(Sp, Xb[1 - u], k + 1)
            elif Sn is not None:
                gather(Sn, Xb[1 - u], 0)
            if Sn is not None:
                act(Sn, k)
        point(Db[1], NB - 1)
        pool(NB - 1)
        d_ref[RC - 1] = hmax(PV.at[0], jnp.maximum(o_ref[R - 2], o_ref[R - 1]), W)

    @pl.when(b == 0)
    def _():
        borders(S0)

        @loop(NB)
        def _(k):
            act(S0, k)
        gather(S0, X0, 0)

    inner = (b > 0) & (b < B)

    @pl.when(inner & (b % 2 == 0))
    def _():
        step(S0, S1)

    @pl.when(inner & (b % 2 == 1))
    def _():
        step(S1, S0)

    @pl.when(b == B)
    def _():
        step(None, S1)

    @pl.when(b > 0)
    def _():
        h_ref[0] = hmax(PV.at[0], o_ref[0], W)

        a = coefs(two, three, TOP)
        maps = (p4_ref[0], t4_ref[0], d_ref[0])
        h_ref[1] = swish(sum(x.astype(f32) * y for x, y in zip(maps, a))).astype(bf16)


def call_fine(two, three, p, ph, t, p4, wts):
    def block(s, late=False, row=0):
        return pl.BlockSpec((None,) + s[1:], lambda b: (prev(b) if late else jnp.minimum(b, B - 1), row, 0, 0))
    full = [pl.BlockSpec(a.shape, lambda b, n=a.ndim: (0,) * n) for a in wts]
    outs = [shape(3, R3), shape(4, RC3), shape(4, 2)]
    S = vm((1, 2, R3 + 2, W3 + 2 * TILE, H), f32)
    X = vm((2, PB * W3 + TILE, K3))
    D = vm((2 * PB * W3 + TILE, C))
    return pl.pallas_call(
        fine, grid=(B + 1,),
        out_shape=[struct(s) for s in outs],
        in_specs=[SMEM] * 2 + [block(a.shape) for a in (p, ph, t)] + [block(shape(4, 1), True, r) for r in TWO] + full,
        out_specs=[block(s, True) for s in outs],
        scratch_shapes=[S, S, vm((2, 2, W3, H), f32), X, X, D, D, vm((PB, 2, W3 + TILE, H), f32), vm((2, K3, C)), vm((9, TILE, C), f32)],
        compiler_params=pltpu.CompilerParams(vmem_limit_bytes=60 * MIB),
    )(two, three, p, ph, t, p4, t, *wts)


def bottom_up(*refs, n_dev):
    take = splitter(refs)
    two, three, p4 = take(3)
    Ph = {4: p4, **dict(zip(LOW, take(3)))}
    Xh, Th = dict(zip(LV, take(4))), dict(zip(TD, take(3)))
    d4, h4, dw_ref, pw_ref, sc_ref, bi_ref = take(6)
    Oh = dict(zip(LV, take(4)))
    Pv, Tv, Dv, Ov = dict(zip(LV, take(4))), dict(zip(TD, take(3))), dict(zip(LV, take(4))), dict(zip(LV, take(4)))
    UP, UR, DR, S = [dict(zip(LV, take(4))) for _ in range(4)]
    V = dict(zip(TD, take(3)))
    F = dict(zip(LOW, take(3)))
    D, DW, ls, os, s_up, r_up, s_dn, r_dn = take(8)
    me = lax.axis_index('sp')
    last = n_dev - 1
    wts = (DW, pw_ref, sc_ref, bi_ref)

    def sl(g):
        return pl.ds(g * N, N)

    def loads(l, g):
        q = sl(g)
        pairs = [(Xh[l].at[q], Pv[l].at[q, ROW0])]
        if l == TOP:
            pairs += [(p4.at[q], Pv[4].at[q, pl.ds(1, ROWS[4])]), (d4.at[q], Dv[4].at[q]), (h4.at[q], UP[4].at[q])]
        if l < END:
            pairs += [(Th[l].at[q], Tv[l].at[q])]
        return [pltpu.make_async_copy(a, b, ls.at[l - TOP, g, i]) for i, (a, b) in enumerate(pairs)]

    def up(l, g):
        return remote((h4 if l == TOP else UP[l]).at[sl(g)], UR[l].at[sl(g)], s_up.at[l - TOP, g], r_up.at[l - TOP, g], me - 1)

    def dn(l, g):
        return remote((d4 if l == TOP else Dv[l]).at[sl(g), pl.ds(ROWS[l] - 1, 1)], DR[l].at[sl(g)], s_dn.at[l - TOP, g], r_dn.at[l - TOP, g], me + 1)

    def send(l, g):
        @pl.when(me > 0)
        def _():
            up(l, g).start()

        @pl.when(me < last)
        def _():
            dn(l, g).start()

    def arrive(l, g):
        @pl.when(me < last)
        def _():
            up(l, g).wait_recv()

        @pl.when(me > 0)
        def _():
            dn(l, g).wait_recv()

    CF = {l: coefs(two, three, l) for l in LV}

    def fuse(l, b, r, d):
        a = CF[l]
        h = Pv[l][b, r + 1].astype(f32) * a[0] + d.astype(f32) * a[-1]
        if l < END:
            h = h + Tv[l][b, r + 1].astype(f32) * a[1]
        return h

    def first(l, b):
        UP[l][b, 1] = swish(fuse(l, b, 0, Dv[l][b, 0])).astype(bf16)

    barrier_signal(me, last)

    @groups
    def _(g):
        for l in LV:
            for c in loads(l, g):
                c.start()
    barrier_wait(me, last)

    @groups
    def _(g):
        send(4, g)
    widen(dw_ref, DW)
    for l in LV:
        zero_edges(S[l], COLS[l])
        if l < END:
            V[l][:, COLS[l]:COLS[l] + TILE, :] = jnp.full((2, TILE, H), NEG, f32)

    @pl.when(me == last)
    def _():
        for l in LV:
            UR[l][:, :1] = jnp.full(shape(l, 1), NEG, bf16)
            UR[l][:, 1:] = jnp.zeros(shape(l, 1), bf16)

    @pl.when(me == 0)
    def _():
        for l in LV:
            DR[l][...] = jnp.zeros(shape(l, 1), bf16)

    for l in LOW:
        rows_first(l, Ph[l], Pv[l], 1, F[l])

    def node(l, g):
        W, R = COLS[l], ROWS[l]
        nb = SLOTS[l]

        def borders(b, ib):
            put_s(S[l], ib, 0, W, fuse(l, b, -1, jnp.maximum(DR[l][b, 0], UP[l][b, 0])))
            put_s(S[l], ib, R, W, fuse(l, b, R - 1, jnp.maximum(Dv[l][b, R - 1], UR[l][b, 0])))
            for c, v in enumerate(halves(UR[l][b, 1].astype(f32))):
                S[l][ib, c, R + 1, cols(W), :] = v

            @pl.when(me == 0)
            def _():
                S[l][ib, :, 0, cols(W), :] = jnp.zeros((2, W, H), f32)

        def pools(b):
            n = R // 2

            def row(r):
                return Ov[l][b, r]
            UP[l + 1][b, 0] = hmax(V[l], row(0), W)

            def pooled(r, inner):
                m = jnp.maximum(row(2 * r), row(2 * r + 1))
                if inner:
                    m = jnp.maximum(m, row(2 * r + 2))
                Dv[l + 1][b, r] = hmax(V[l], m, W)
            if l == TOP:
                @loop(n - 1)
                def _(r):
                    pooled(r, True)
            else:
                for r in range(n - 1):
                    pooled(r, True)
            pooled(n - 1, False)
            first(l + 1, b)

        def before(i):
            b0 = g * N + i * nb
            for ib in range(nb):
                borders(b0 + ib, ib)
            if l == TOP:
                @loop(len(THREE))
                def _(q):
                    for y in range(5):
                        r = 5 * q + y
                        put_s(S[l], 0, r + 1, W, fuse(l, b0, r, Dv[l][b0, r]))
            else:
                for ib in range(nb):
                    for r in range(R - 1):
                        put_s(S[l], ib, r + 1, W, fuse(l, b0 + ib, r, Dv[l][b0 + ib, r]))

        def put(i, ib, o, v):
            Ov[l][g * N + i * nb + ib, o] = v

        def after(i):
            for ib in range(nb):
                pools(g * N + i * nb + ib)
        nq = 2 if l == TOP else 1
        lagged(l, l, N // nb, nq, R // nq, S[l], D, wts, before, put, after if l < END else None)

    def out(l, g):
        return pltpu.make_async_copy(Ov[l].at[sl(g)], Oh[l].at[sl(g)], os.at[l - TOP, g])

    for l in LV:
        @groups
        def _(g):
            if l == TOP:
                for c in loads(l, g):
                    c.wait()
            if l < END:
                for c in loads(l + 1, g):
                    c.wait()
            arrive(l, g)
            node(l, g)
            if l < END:
                send(l + 1, g)
            out(l, g).start()

    for cond, cp in ((me > 0, up), (me < last, dn)):
        @pl.when(cond)
        def _(cp=cp):
            @groups
            def _(g):
                for l in LV:
                    cp(l, g).wait_send()

    @groups
    def _(g):
        for l in LV:
            out(l, g).wait()


def call_bottom_up(n_dev, two, three, p4, qs, xs, ts, d4, h4, wts):
    scratch = [vm(shape(l, ROWS[l] + 1)) for l in LV] + [vm(shape(l, ROWS[l] + 2)) for l in TD]
    scratch += [vm(shape(l, ROWS[l])) for l in LV] * 2 + [vm(shape(l, 2)) for l in LV] * 2 + [vm(shape(l, 1)) for l in LV]
    scratch += [vm((SLOTS[l], 2, ROWS[l] + 2, PADC[l] + 2 * TILE, H), f32) for l in LV] + [vm((2, PADC[l] + TILE, H), f32) for l in TD]
    scratch += [flip_buffer(l) for l in LOW]
    scratch += [product_rows(), vm((9, TILE, C), f32), DMA((4, G, 5))] + [DMA((4, G))] * 5
    return pl.pallas_call(
        functools.partial(bottom_up, n_dev=n_dev),
        out_shape=[struct(shape(l, ROWS[l])) for l in LV],
        in_specs=[SMEM] * 2 + [ANY] + [VMEM] * 3 + [ANY] * 9 + [VMEM] * 4,
        out_specs=[ANY] * 4,
        scratch_shapes=scratch,
        compiler_params=pltpu.CompilerParams(collective_id=1, has_side_effects=True, vmem_limit_bytes=62 * MIB),
    )(two, three, p4, *qs, *xs, *ts, d4, h4, *wts)


def finish(*refs):
    take = splitter(refs)
    src, dst, got, put, F = [dict(zip(LV, take(4))) for _ in range(4)] + [dict(zip(LOW, take(3)))]
    si, so, ti, to = take(4)
    top = got[TOP]

    def piece(g):
        return pl.ds(TWO_N * g, TWO_N)

    def cin(g):
        return pltpu.make_async_copy(src[TOP].at[piece(g)], top.at[piece(g)], si.at[g])

    def cout(g):
        return pltpu.make_async_copy(top.at[piece(g)], dst[TOP].at[piece(g)], so.at[g])

    def small_in(l):
        return pltpu.make_async_copy(src[l], got[l], ti.at[l - TOP])

    def small_out(l):
        return pltpu.make_async_copy(put[l], dst[l], to.at[l - TOP])

    for l in LOW[::-1]:
        small_in(l).start()

    @loop(CHUNKS)
    def _(g):
        cin(g).start()
    for l in LOW[::-1]:
        W, R, st = COLS[l], ROWS[l], COLS[l] + 1
        small_in(l).wait()

        @loop(CHUNKS)
        def _(i):
            if l == LOW[0]:
                cin(i).wait()
                cout(i).start()
            for d in TWO:
                b = 2 * i + d
                for r in range(R):
                    for c, v in enumerate(halves(got[l][b, r].astype(f32))):
                        F[l][d, c, r * st:r * st + W, :] = v
                for w in range(W):
                    put[l][b, w] = join([F[l][d, c, pl.ds(w, R, stride=st), :] for c in TWO]).astype(bf16)
        small_out(l).start()
    for l in LOW:
        small_out(l).wait()

    @loop(CHUNKS)
    def _(g):
        cout(g).wait()


def call_finish(ins):
    outs = [shape(4, ROWS[4])] + [flipped(l) for l in LOW]
    return pl.pallas_call(
        finish,
        out_shape=[struct(x) for x in outs],
        in_specs=[ANY] * 4,
        out_specs=[ANY] * 4,
        scratch_shapes=[vm(a.shape) for a in ins] + [vm((TILE, H))] + [vm(x) for x in outs[1:]] + [flip_buffer(l) for l in LOW]
        + [DMA((CHUNKS,))] * 2 + [DMA((4,))] * 2,
        compiler_params=pltpu.CompilerParams(vmem_limit_bytes=62 * MIB),
    )(*ins)


def flip(a):
    return jnp.swapaxes(a, 1, 2)


def solution(mesh):
    n_dev = mesh.shape['sp']

    def body(p3, p4, p5, p6, p7, fuse_two, fuse_three, dw_filter, pw_weight, bn_scale, bn_bias):
        two, three = fuse_two.T, fuse_three
        qs = [flip(a) for a in (p5, p6, p7)]
        wts = (jnp.transpose(dw_filter, (1, 2, 0, 3)), pw_weight, bn_scale, bn_bias)
        t4, t5, t6, h3, *xs = call_top_down(n_dev, two, three, p3, p4, qs, wts)
        out3, d4, h4 = call_fine(two, three, p3, h3, t4, p4, wts)
        outs = call_bottom_up(n_dev, two, three, p4, qs, xs, (t4, t5, t6), d4, h4, wts)
        out4, *rest = call_finish(outs)
        return out3, out4, *[flip(a) for a in rest]

    band_spec = P('dp', 'sp')
    whole = P()
    return jax.shard_map(body, mesh=mesh, in_specs=(band_spec,) * 5 + (whole,) * 6, out_specs=(band_spec,) * 5, check_vma=False)
```
